32 devices in a mesh: aux: 8 (over y, x, core), pair: 4 (over z).
Axes of the slice: x: 2, y: 2, z: 4, core: 2. Of those that a mesh axis runs over, the one named last changes fastest.
Arguments:
- integrals: bfloat16 [3072, 32768], P('aux', 'pair'), may hold values from -0.15625 to 0.15625
- densities: bfloat16 [16, 32768], P(None, 'pair'), may hold values from -2.390625 to 2.390625
- screen: int32 [24, 256], P('aux', 'pair'), may hold values 0 or 1
- factor: float32 [3072, 3072], P('aux', 'pair'), may hold values from -0.109375 to 0.109375
- diag_inv: float32 [3072, 768], P('aux'), may hold values from -2 to 2, as said below
Outputs:
- coulomb: float32 [16, 32768], P(None, ('pair', 'aux'))
The draws below stay inside these ranges and needn't reach their ends.
Inputs may be any that keep to these rules, and one draw needn't show every extreme that they name: `diag_inv`: each block of 768 rows is an upper triangular matrix with a positive diagonal.
All inputs are finite; a program needn't handle non-finite values. No bound on the sum of `screen` on one device may be relied on, other than what follows from the above.
Results may differ from the reference program's by a relative error of at most 0.0041.
Values may be sent and summed in bfloat16 or wider, within the bound.
A program may use at most 128 MiB of HBM per device.

```python
import math
import jax
import jax.numpy as jnp
from jax import lax

AUX_DEV = 384
DENS = 16
TILE = 128
SOLVE_BLOCKS = 4
NAUX = 3072
BLOCK = 768
NPAIR = 32768


def draw_diag_inv(key, part):
    off_key = jax.random.fold_in(key, 11)
    diag_key = jax.random.fold_in(key, 12)
    spread = 0.5 / math.sqrt(BLOCK)
    offdiag = jnp.clip(jax.random.normal(off_key, (NAUX, BLOCK), jnp.float32), -4.0, 4.0) * spread
    diagonal = jnp.exp(jax.random.uniform(diag_key, (NAUX, 1), jnp.float32, math.log(0.7), math.log(1.4)))
    within = (jnp.arange(NAUX, dtype=jnp.int32) % BLOCK)[:, None]
    across = jnp.arange(BLOCK, dtype=jnp.int32)[None, :]
    return jnp.where(across == within, diagonal, jnp.where(across > within, offdiag, 0.0)).astype(jnp.float32)


def set_ends(result, own_key, low, largest):
    extent = result.shape
    index_at = [jax.random.randint(jax.random.fold_in(own_key, axis), (), 0, extent[axis]) for axis in range(len(extent))]
    result = result.at[tuple(index_at)].set(low)
    longest = extent.index(max(extent))
    index_at[longest] = (index_at[longest] + 1) % extent[longest]
    return result.at[tuple(index_at)].set(largest)


def spiked(result, rng, source, target, parts, factor):
    owner, partner = [(jnp.arange(result.shape[axis_at]) // (result.shape[axis_at] // parts)).reshape([-1 if axis == axis_at else 1 for axis in range(result.ndim)]) for axis_at in (source, target)]
    chosen = jax.random.permutation(rng, parts)[partner]
    strong = (owner == chosen) | (owner == (partner + parts // 2) % parts)
    return jnp.where(strong, factor * result, result)


def shard_levels(rng, dims, shards, smallest, high):
    gain = 1.0
    for dim, shards_of in shards:
        heights = jax.random.uniform(jax.random.fold_in(jax.random.fold_in(rng, 6), dim), (shards_of,), jnp.float32, smallest / len(shards), high / len(shards))
        gain = gain * jnp.repeat(jnp.exp(heights), dims[dim] // shards_of).reshape((-1,) + (1,) * (len(dims) - 1 - dim))
    return gain


def noise(rng, extent, width, bound, split=(), held_as=jnp.bfloat16):
    level = shard_levels(rng, extent, split, -0.22, 0.18) if split else 1.0
    array = jax.random.normal(rng, extent, jnp.float32) * width * level
    return jnp.minimum(jnp.maximum(array, -bound), bound).astype(held_as)


def heavy_noise(own_key, dims, width, reach, shards, heavy, kind=jnp.bfloat16):
    entries = width * jax.random.normal(own_key, dims, jnp.float32)
    if shards:
        entries = entries * shard_levels(own_key, dims, shards, -0.22, 0.18)
    return jnp.clip(spiked(entries, jax.random.fold_in(own_key, 3), *heavy), -reach, reach).astype(kind)


def setup_inputs(seed: int = 0) -> dict:
    key_list = jax.random.split(jax.random.key(seed), 6)
    integrals = heavy_noise(key_list[0], (NAUX, NPAIR), NAUX ** -0.5, 0.15625, ((0, 8), (1, 4)), (0, 1, 8, 2.0))
    densities = noise(key_list[1], (DENS, NPAIR), 0.4, 2.390625, ((1, 4),))
    screen = set_ends((jax.random.randint(key_list[2], (NAUX // TILE, NPAIR // TILE), 0, 4) < 3).astype(jnp.int32), jax.random.fold_in(key_list[2], 1), 0, 1)
    factor = noise(key_list[3], (NAUX, NAUX), NAUX ** -0.5, 0.109375, ((0, 8), (1, 4)), jnp.float32)
    diag_inv = draw_diag_inv(jax.random.fold_in(key_list[5], 71), 0)
    return dict(integrals=integrals, densities=densities, screen=screen, factor=factor, diag_inv=diag_inv)


def reference(integrals, densities, screen, factor, diag_inv):
    blocks = NAUX // AUX_DEV
    highest = lax.Precision.HIGHEST
    tiles_block = AUX_DEV // TILE

    def masked_rows(index):
        slab_rows = lax.dynamic_slice_in_dim(integrals, index * AUX_DEV, AUX_DEV, 0)
        screen_tiles = lax.dynamic_slice_in_dim(screen, index * tiles_block, tiles_block, 0)
        expanded = jnp.repeat(jnp.repeat(screen_tiles, TILE, axis=0), TILE, axis=1).astype(jnp.bfloat16)
        return slab_rows * expanded

    def fit_block(index):
        return lax.dot_general(densities, masked_rows(index), (((1,), (1,)), ((), ())), preferred_element_type=jnp.float32)

    fitted_blocks = lax.map(fit_block, jnp.arange(blocks, dtype=jnp.int32))
    fitted = jnp.transpose(fitted_blocks, (1, 0, 2)).reshape(DENS, NAUX)

    solved = jnp.zeros((DENS, NAUX), jnp.float32)
    for k in range(SOLVE_BLOCKS):
        offset = k * BLOCK
        upper = offset + BLOCK
        residual = fitted[:, offset:upper]
        if k > 0:
            residual = residual - jnp.dot(solved[:, :offset], factor[offset:upper, :offset].T, precision=highest, preferred_element_type=jnp.float32)
        solved = solved.at[:, offset:upper].set(jnp.dot(residual, diag_inv[offset:upper], precision=highest, preferred_element_type=jnp.float32))

    coefficients = jnp.zeros((DENS, NAUX), jnp.float32)
    for k in reversed(range(SOLVE_BLOCKS)):
        offset = k * BLOCK
        upper = offset + BLOCK
        residual = solved[:, offset:upper]
        if upper < NAUX:
            residual = residual - jnp.dot(coefficients[:, upper:], factor[upper:, offset:upper], precision=highest, preferred_element_type=jnp.float32)
        coefficients = coefficients.at[:, offset:upper].set(jnp.dot(residual, diag_inv[offset:upper].T, precision=highest, preferred_element_type=jnp.float32))

    rounded = coefficients.astype(jnp.bfloat16)

    def add_block(running, index):
        weights = lax.dynamic_slice_in_dim(rounded, index * AUX_DEV, AUX_DEV, 1)
        return running + jnp.dot(weights, masked_rows(index), preferred_element_type=jnp.float32), None

    coulomb, unused = lax.scan(add_block, jnp.zeros((DENS, NPAIR), jnp.float32), jnp.arange(blocks, dtype=jnp.int32))
    return coulomb
```

```python
import functools

import jax
import jax.numpy as jnp
from jax import lax
from jax.experimental import pallas as pl
from jax.experimental.pallas import tpu as pltpu
from jax.sharding import PartitionSpec as P

TILE = 128
SOLVE_BLOCKS = 4
STREAM = 1024
VMEM_ROOM = 48 * 2**20
MESH = pl.DeviceIdType.MESH
NN = (((1,), (0,)), ((), ()))
NT = (((1,), (1,)), ((), ()))
F32 = jnp.float32
BF16 = jnp.bfloat16
P_KIND, S_KIND, U_KIND, V_KIND, L_KIND = BF16, BF16, F32, BF16, BF16


def split(values):
    high = values.astype(BF16)
    return high, (values - high.astype(F32)).astype(BF16)


def dot_split(values, high, low, dims):
    top, rest = split(values)
    rows = values.shape[0]
    both = lax.dot_general(
        jnp.concatenate([top, rest], 0), high, dims, preferred_element_type=F32
    )
    minor = lax.dot_general(top, low, dims, preferred_element_type=F32)
    return both[:rows] + (both[rows:] + minor)


def spread_kernel(
    n_aux, n_pair,
    integrals, densities, screen, factor, diag_inv, out,
    masked, dens, fac, inv, fac_hi, fac_lo, inv_hi, inv_lo,
    fit_out, fit_in, u_out, u_in, s_out, s_in, s_sum, own_in, resid, coef, v_out, v_in,
    part_out, part_in,
    load_sem, small_sem,
    fit_send, fit_recv, u_send, u_recv, s_send, s_recv, own_send, own_recv,
    coef_send, coef_recv, v_send, v_recv, part_send, part_recv,
):
    height, width = masked.shape
    breadth = fac.shape[1]
    block = inv.shape[1]
    members = block // height
    group = block // breadth
    pieces = breadth // height
    share = width // n_aux
    chunks = width // STREAM

    row = lax.axis_index("aux")
    col = lax.axis_index("pair")
    mine = row // members
    member = lax.rem(row, members)
    column_block = col // group
    column_part = lax.rem(col, group)

    def home_of(k):
        return jnp.maximum(k - 1, 0) * group

    home = home_of(mine)
    is_home = col == home
    below = column_block < mine

    def remote(src, dst, send, recv, aux, pair):
        return pltpu.make_async_remote_copy(
            src_ref=src, dst_ref=dst, send_sem=send, recv_sem=recv,
            device_id={"aux": aux, "pair": pair}, device_id_type=MESH,
        )

    def load(c):
        at = pl.ds(pl.multiple_of(c * STREAM, STREAM), STREAM)
        return pltpu.make_async_copy(integrals.at[:, at], masked.at[:, at], load_sem.at[c])

    load_dens = pltpu.make_async_copy(densities, dens, small_sem.at[0])
    load_fac = pltpu.make_async_copy(factor, fac, small_sem.at[1])
    load_inv = pltpu.make_async_copy(diag_inv, inv, small_sem.at[2])
    load_dens.start()
    for c in range(chunks):
        load(c).start()
    load_inv.start()

    @pl.when(below)
    def _():
        load_fac.start()

    barrier = pltpu.get_barrier_semaphore()
    everyone = n_aux * n_pair
    me = row * n_pair + col

    def greet(i, carry):
        other = lax.rem(me + i, everyone)
        pl.semaphore_signal(
            barrier, inc=1,
            device_id={"aux": other // n_pair, "pair": lax.rem(other, n_pair)},
            device_id_type=MESH,
        )
        return carry

    lax.fori_loop(1, everyone, greet, 0)
    load_dens.wait()

    def fit_step(c, total):
        load(c).wait()
        base = pl.multiple_of(c * STREAM, STREAM)
        for r in range(height // TILE):
            for t in range(STREAM // TILE):
                flag = screen[r, c * (STREAM // TILE) + t].astype(F32)
                at = (pl.ds(r * TILE, TILE), pl.ds(pl.multiple_of(base + t * TILE, TILE), TILE))
                masked[at] = masked[at] * jnp.full((TILE, TILE), flag, F32).astype(BF16)
        span = pl.ds(base, STREAM)
        return total + lax.dot_general(
            dens[:, span], masked[:, span], NT, preferred_element_type=F32
        )

    fitted = lax.fori_loop(0, chunks, fit_step, jnp.zeros((dens.shape[0], height), F32))
    fit_out[...] = fitted
    pl.semaphore_wait(barrier, everyone - 1)

    send_fit = remote(fit_out, fit_in.at[col], fit_send, fit_recv.at[col], row, home)

    @pl.when(jnp.logical_not(is_home))
    def _():
        send_fit.start()

    load_inv.wait()
    high, low = split(inv[...])
    inv_hi[...] = high
    inv_lo[...] = low

    @pl.when(below)
    def _():
        load_fac.wait()
        high, low = split(fac[...])
        fac_hi[...] = high
        fac_lo[...] = low

    @pl.when(below)
    def _():
        for x in range(pieces):
            whole_x = column_part * pieces + x
            for c in range(members):
                @pl.when(whole_x >= c)
                def _():
                    remote(s_out.at[0], s_in.at[c, x], s_send.at[0, 0], s_recv.at[c, x], row, col).wait_recv()
                    if c == 0:
                        s_sum[x] = s_in[c, x]
                    else:
                        s_sum[x] += s_in[c, x]
        known = jnp.concatenate([s_sum[x] for x in range(pieces)], 1)
        u_out[...] = dot_split(known, fac_hi[...], fac_lo[...], NT)

        @pl.when(jnp.logical_not(is_home))
        def _():
            remote(u_out, u_in.at[col], u_send, u_recv.at[col], row, home).start()

    def send_solved(x, start):
        part, piece = x // pieces, x % pieces

        def later(d, carry):
            copy = remote(
                s_out.at[x], s_in.at[member, piece], s_send.at[x, d],
                s_recv.at[member, piece], d, mine * group + part,
            )
            copy.start() if start else copy.wait_send()
            return carry

        lax.fori_loop((mine + 1) * members, n_aux, later, 0)
        for i in range(1, members):
            other = lax.rem(member + i, members)

            @pl.when(other <= x)
            def _():
                copy = remote(
                    s_out.at[x], own_in.at[member, x], own_send.at[x, i],
                    own_recv.at[member, x], mine * members + other, home,
                )
                copy.start() if start else copy.wait_send()

    @pl.when(is_home)
    def _():
        fit_total = fit_out
        for p in range(n_pair):
            @pl.when(p != home)
            def _():
                remote(fit_out, fit_in.at[p], fit_send, fit_recv.at[p], row, col).wait_recv()
                fit_total[...] += fit_in[p]
        for p in range(n_pair):
            @pl.when(jnp.logical_and(p // group < mine, p != home))
            def _():
                remote(u_out, u_in.at[p], u_send, u_recv.at[p], row, col).wait_recv()
                fit_total[...] -= u_in[p]

        @pl.when(below)
        def _():
            fit_total[...] -= u_out[...]

        for x in range(members):
            @pl.when(x >= member)
            def _():
                at = pl.ds(x * height, height)
                s_out[x] = dot_split(fit_total[...], inv_hi[:, at], inv_lo[:, at], NN)
                send_solved(x, True)

        for x in range(members):
            @pl.when(x >= member)
            def _():
                resid[x] = s_out[x]
                for i in range(1, members):
                    other = lax.rem(member + i, members)

                    @pl.when(other <= x)
                    def _():
                        remote(s_out.at[0], own_in.at[other, x], own_send.at[0, 0], own_recv.at[other, x], row, col).wait_recv()
                        resid[x] += own_in[other, x]

        def subtract(i, carry):
            source = n_aux - 1 - i
            for x in range(members):
                @pl.when(x >= member)
                def _():
                    remote(v_out.at[0], v_in.at[source, x], v_send.at[0, 0], v_recv.at[source, x], row, col).wait_recv()
                    resid[x] -= v_in[source, x]
            return carry

        lax.fori_loop(0, n_aux - (mine + 1) * members, subtract, 0)
        for x in reversed(range(members)):
            @pl.when(x >= member)
            def _():
                at = pl.ds(x * height, height)
                term = dot_split(resid[x], inv_hi[:, at], inv_lo[:, at], NT)
                if x == members - 1:
                    coef[...] = term
                else:
                    coef[...] += term

        for i in range(1, n_pair):
            remote(coef, coef, coef_send.at[i], coef_recv, row, lax.rem(col + i, n_pair)).start()

    @pl.when(jnp.logical_not(is_home))
    def _():
        remote(coef, coef, coef_send.at[0], coef_recv, row, col).wait_recv()

    def send_v(x, start):
        whole_x = column_part * pieces + x
        for c in range(members):
            @pl.when(c <= whole_x)
            def _():
                copy = remote(
                    v_out.at[x], v_in.at[row, whole_x], v_send.at[x, c],
                    v_recv.at[row, whole_x], column_block * members + c, home_of(column_block),
                )
                copy.start() if start else copy.wait_send()

    @pl.when(below)
    def _():
        for x in range(pieces):
            at = pl.ds(x * height, height)
            v_out[x] = dot_split(coef[...], fac_hi[:, at], fac_lo[:, at], NN)
            send_v(x, True)

    rounded = coef[...].astype(BF16)

    def product(target):
        span = pl.ds(pl.multiple_of(target * share, TILE), share)
        return lax.dot_general(rounded, masked[:, span], NN, preferred_element_type=F32)

    def part_copy(i):
        target = lax.rem(row + i, n_aux)
        return target, remote(
            part_out.at[target], part_in.at[row], part_send.at[target], part_recv.at[row], target, col
        )

    def give(i, carry):
        target, copy = part_copy(i)
        part_out[target] = product(target).astype(BF16)
        copy.start()
        return carry

    lax.fori_loop(1, n_aux, give, 0)
    total = product(row)

    def take(i, total):
        source = lax.rem(row + n_aux - i, n_aux)
        remote(part_out.at[0], part_in.at[source], part_send.at[0], part_recv.at[source], row, col).wait_recv()
        return total + part_in[source].astype(F32)

    out[...] = lax.fori_loop(1, n_aux, take, total)

    @pl.when(jnp.logical_not(is_home))
    def _():
        send_fit.wait_send()

        @pl.when(below)
        def _():
            remote(u_out, u_in.at[col], u_send, u_recv.at[col], row, home).wait_send()

    @pl.when(is_home)
    def _():
        for x in range(members):
            @pl.when(x >= member)
            def _():
                send_solved(x, False)
        for i in range(1, n_pair):
            remote(coef, coef, coef_send.at[i], coef_recv, row, lax.rem(col + i, n_pair)).wait_send()

    @pl.when(below)
    def _():
        for x in range(pieces):
            send_v(x, False)

    def sent(i, carry):
        part_copy(i)[1].wait_send()
        return carry

    lax.fori_loop(1, n_aux, sent, 0)


def dot_two(values, high, low, dims):
    return lax.dot_general(values, high, dims, preferred_element_type=F32) + lax.dot_general(
        values, low, dims, preferred_element_type=F32
    )


def apply(values, high, low, dims):
    return (dot_two if values.dtype == BF16 else dot_split)(values, high, low, dims)


def lead_kernel(
    n_aux, n_pair,
    integrals, densities, screen, factor, diag_inv, out,
    flags, masked, dens, fac, inv, fac_hi, fac_lo, inv_hi, inv_lo, inv_t_hi, inv_t_lo,
    step_hi, step_lo, step_t_hi, step_t_lo,
    fit_out, fit_in, p_out, p_in, u_out, u_in, s_out, s_in, w_out, w_in, v_out, v_in,
    resid, solved, start, rounded, last_out, last_in, part_out, part_in,
    load_sem, small_sem, fac_send, fac_recv, inv_send, inv_recv,
    fit_send, fit_recv, p_send, p_recv, u_send, u_recv, s_send, s_recv, w_send, w_recv,
    v_send, v_recv, round_send, round_recv, last_send, last_recv, part_send, part_recv,
):
    height, width = masked.shape
    block = inv.shape[1]
    count = dens.shape[0]
    members = block // height
    share = width // n_aux
    chunks = width // STREAM
    strips = height // TILE

    row = lax.axis_index("aux")
    col = lax.axis_index("pair")
    mine = row // members
    member = lax.rem(row, members)
    lead = members - 1
    lead_row = mine * members + lead
    is_lead = member == lead
    first = mine == 0
    later = mine > 0
    home = jnp.maximum(mine - 1, 0)
    at_home = jnp.logical_and(later, col == home)
    below = col < mine

    def chip(k, z):
        return jnp.logical_and(mine == k, col == z)

    def role(k, z):
        return jnp.logical_and(is_lead, chip(k, z))

    lead_home = jnp.logical_and(is_lead, at_home)
    lead_below = jnp.logical_and(is_lead, below)
    with_inv = jnp.logical_or(at_home, chip(2, 0))

    def remote(src, dst, send, recv, aux, pair):
        return pltpu.make_async_remote_copy(
            src_ref=src, dst_ref=dst, send_sem=send, recv_sem=recv,
            device_id={"aux": aux, "pair": pair}, device_id_type=MESH,
        )

    def to_lead(src, dst, send, recv, k, z):
        return remote(src, dst, send, recv, k * members + lead, z)

    def load(c):
        at = pl.ds(pl.multiple_of(c * STREAM, STREAM), STREAM)
        return pltpu.make_async_copy(integrals.at[:, at], masked.at[:, at], load_sem.at[c])

    own = pl.ds(lead * height, height)
    load_dens = pltpu.make_async_copy(densities, dens, small_sem.at[0])
    load_fac = pltpu.make_async_copy(factor, fac.at[own], small_sem.at[1])
    load_inv = pltpu.make_async_copy(diag_inv, inv.at[own], small_sem.at[2])
    load_flags = pltpu.make_async_copy(screen, flags, small_sem.at[3])

    def move_fac(c):
        return remote(factor, fac.at[pl.ds(c * height, height)], fac_send, fac_recv.at[c], lead_row, col)

    def move_inv(c):
        right = pl.ds(c * height, block - c * height)
        return remote(
            diag_inv.at[:, right], inv.at[pl.ds(c * height, height), right],
            inv_send, inv_recv.at[c], lead_row, col,
        )

    lead_inv = jnp.logical_and(is_lead, with_inv)
    load_flags.start()
    load_dens.start()

    @pl.when(first)
    def _():
        load_inv.start()

    for c in range(chunks):
        load(c).start()

    @pl.when(lead_inv)
    def _():
        load_inv.start()
        for c in range(1, lead):
            inv[pl.ds(c * height, height), pl.ds(0, c * height)] = jnp.zeros((height, c * height), F32)

    @pl.when(lead_below)
    def _():
        load_fac.start()

    barrier = pltpu.get_barrier_semaphore()
    everyone = n_aux * n_pair
    me = row * n_pair + col

    def greet(i, carry):
        other = lax.rem(me + i, everyone)
        pl.semaphore_signal(
            barrier, inc=1,
            device_id={"aux": other // n_pair, "pair": lax.rem(other, n_pair)},
            device_id_type=MESH,
        )
        return carry

    lax.fori_loop(1, everyone, greet, 0)

    @pl.when(first)
    def _():
        load_inv.wait()
        inv_hi[own], inv_lo[own] = split(inv[own])

    load_flags.wait()
    load_dens.wait()

    def flag_of(r, t):
        return flags[r, t].astype(F32)

    def fit_step(c, total):
        base = pl.multiple_of(c * STREAM, STREAM)
        kept = []
        for r in range(strips):
            tiles = []
            for t in range(STREAM // TILE):
                at = pl.ds(pl.multiple_of(base + t * TILE, TILE), TILE)
                flag = flag_of(r, c * (STREAM // TILE) + t)
                tiles.append(dens[:, at] * jnp.full((count, TILE), flag, F32).astype(BF16))
            kept.append(jnp.concatenate(tiles, 1))
        load(c).wait()
        return total + lax.dot_general(
            jnp.concatenate(kept, 0), masked[:, pl.ds(base, STREAM)], NT, preferred_element_type=F32
        )

    total = lax.fori_loop(0, chunks, fit_step, jnp.zeros((strips * count, height), F32))
    for r in range(strips):
        at = slice(r * TILE, (r + 1) * TILE)
        fit_out[:, at] = total[r * count:(r + 1) * count, at]

    p_targets = ((1, 0), (2, 0))

    def send_p(c, i):
        right = pl.ds(c * height, block - c * height)
        return to_lead(
            p_out.at[:, right], p_in.at[col, c, :, right], p_send.at[i], p_recv.at[col, c], *p_targets[i]
        )

    for c in range(members):
        @pl.when(jnp.logical_and(first, member == c))
        def _():
            right = pl.ds(c * height, block - c * height)
            p_out[:, right] = dot_split(
                fit_out[...], inv_hi[own, right], inv_lo[own, right], NN
            ).astype(p_out.dtype)

    pl.semaphore_wait(barrier, everyone - 1)

    for c in range(members):
        @pl.when(jnp.logical_and(first, member == c))
        def _():
            for i in range(len(p_targets)):
                send_p(c, i).start()

    send_fit = remote(
        fit_out, fit_in.at[col, member], fit_send, fit_recv.at[col, member], lead_row, home
    )
    sends_fit = jnp.logical_and(later, jnp.logical_not(lead_home))

    @pl.when(sends_fit)
    def _():
        send_fit.start()

    for c in range(lead):
        @pl.when(member == c)
        def _():
            @pl.when(below)
            def _():
                move_fac(c).start()

            @pl.when(with_inv)
            def _():
                move_inv(c).start()

    def mask_step(c, carry):
        base = pl.multiple_of(c * STREAM, STREAM)
        for r in range(strips):
            for t in range(STREAM // TILE):
                flag = flag_of(r, c * (STREAM // TILE) + t)
                at = (pl.ds(r * TILE, TILE), pl.ds(pl.multiple_of(base + t * TILE, TILE), TILE))
                masked[at] = masked[at] * jnp.full((TILE, TILE), flag, F32).astype(BF16)
        return carry

    lax.fori_loop(0, chunks, mask_step, 0)

    @pl.when(lead_below)
    def _():
        load_fac.wait()
        for c in range(lead):
            move_fac(c).wait_recv()
        fac_hi[...], fac_lo[...] = split(fac[...])

    @pl.when(lead_inv)
    def _():
        load_inv.wait()
        for c in range(lead):
            move_inv(c).wait_recv()
        inv_hi[...], inv_lo[...] = split(inv[...])

    def prepare_back():
        inv_t_hi[...], inv_t_lo[...] = split(inv[...].T)
        whole = lax.dot_general(inv_t_hi[...], fac_hi[...], NN, preferred_element_type=F32)
        whole += lax.dot_general(inv_t_lo[...], fac_hi[...], NN, preferred_element_type=F32)
        whole += lax.dot_general(inv_t_hi[...], fac_lo[...], NN, preferred_element_type=F32)
        step_t_hi[...], step_t_lo[...] = split(whole)
        return whole

    def gather_fit():
        resid[:, own] = fit_out[...]
        for c in range(lead):
            for p in range(n_pair):
                @pl.when(p == home)
                def _():
                    remote(fit_out, fit_in.at[p, c], fit_send, fit_recv.at[p, c], row, col).wait_recv()
                    resid[:, pl.ds(c * height, height)] = fit_in[p, c]
        for p in range(n_pair):
            for c in range(members):
                @pl.when(p != home)
                def _():
                    remote(fit_out, fit_in.at[p, c], fit_send, fit_recv.at[p, c], row, col).wait_recv()
                    resid[:, pl.ds(c * height, height)] += fit_in[p, c]

    def gather_start():
        for p in range(n_pair):
            for c in range(members):
                right = pl.ds(c * height, block - c * height)
                remote(
                    p_out.at[:, right], p_in.at[p, c, :, right], p_send.at[0], p_recv.at[p, c], row, col
                ).wait_recv()
        for c in range(members):
            at = pl.ds(c * height, height)
            sum_p = p_in[0, 0, :, at].astype(F32)
            for p in range(n_pair):
                for d in range(c + 1):
                    if p or d:
                        sum_p += p_in[p, d, :, at].astype(F32)
            start[:, at] = sum_p

    def send_s(i, slot, k, z):
        return to_lead(s_out.at[slot], s_in, s_send.at[i], s_recv, k, z)

    def send_u(k):
        return to_lead(u_out, u_in.at[col], u_send, u_recv.at[col], k, k - 1)

    def send_v(k, z):
        return to_lead(v_out, v_in.at[mine, col], v_send, v_recv.at[mine, col], k, z)

    def send_w(i, slot, k, z):
        return to_lead(w_out.at[slot], w_in, w_send.at[i], w_recv, k, z)

    def wait_s():
        send_s(0, 0, 0, 0).wait_recv()

    def take_u(p):
        remote(u_out, u_in.at[p], u_send, u_recv.at[p], row, col).wait_recv()
        resid[...] -= u_in[p].astype(F32)

    def take_v(k, z):
        remote(v_out, v_in.at[k, z], v_send, v_recv.at[k, z], row, col).wait_recv()
        return v_in[k, z].astype(F32)

    def wait_w():
        send_w(0, 0, 0, 0).wait_recv()

    def round_copy(k, c, i, z):
        return remote(
            rounded.at[c], rounded.at[c], round_send.at[c, i], round_recv, k * members + c, lax.rem(z + i, n_pair)
        )

    def spread_rounded(k, go):
        for i in reversed(range(n_pair)):
            for c in range(members):
                if c != lead or i:
                    copy = round_copy(k, c, i, k - 1)
                    copy.start() if go else copy.wait_send()

    def finish(k, values):
        coef = dot_split(values, inv_t_hi[...], inv_t_lo[...], NN)
        for c in range(members):
            rounded[c] = coef[:, c * height:(c + 1) * height].astype(BF16)
        spread_rounded(k, True)

    def last_copy(c, z):
        right = pl.ds(c * height, block - c * height)
        return remote(
            last_out.at[:, right], last_in.at[:, right], last_send.at[c, z], last_recv, c, z
        )

    @pl.when(role(1, 0))
    def _():
        gather_fit()
        gather_start()
        s_out[0] = start[...].astype(s_out.dtype)
        send_s(2, 0, 3, 0).start()
        resid[...] -= dot_split(start[...], fac_hi[...], fac_lo[...], NT)
        solved[...] = dot_split(resid[...], inv_hi[...], inv_lo[...], NN)
        s_out[1] = solved[...].astype(s_out.dtype)
        send_s(0, 1, 2, 1).start()
        send_s(1, 1, 3, 1).start()
        prepare_back()
        solved[...] -= take_v(3, 1)
        start[...] -= take_v(3, 0)
        solved[...] -= take_v(2, 1)
        back = apply(solved[...].astype(w_out.dtype), step_t_hi[...], step_t_lo[...], NN)
        last_out[...] = (start[...] - take_v(2, 0) - back).astype(last_out.dtype)
        for z in reversed(range(n_pair)):
            for c in range(members):
                last_copy(c, z).start()
        finish(1, solved[...])

    @pl.when(role(2, 0))
    def _():
        gather_start()
        u_out[...] = dot_split(start[...], fac_hi[...], fac_lo[...], NT).astype(u_out.dtype)
        send_u(2).start()
        prepare_back()
        wait_w()
        v_out[...] = apply(w_in[...], step_t_hi[...], step_t_lo[...], NN).astype(v_out.dtype)
        send_v(1, 0).start()

    @pl.when(jnp.logical_or(role(3, 0), role(3, 1)))
    def _():
        wait_s()
        u_out[...] = apply(s_in[...], fac_hi[...], fac_lo[...], NT).astype(u_out.dtype)
        send_u(3).start()
        wait_w()
        v_out[...] = apply(w_in[...], fac_hi[...], fac_lo[...], NN).astype(v_out.dtype)
        send_v(1, 0).start()

    @pl.when(role(2, 1))
    def _():
        gather_fit()
        take_u(0)
        wait_s()
        resid[...] -= apply(s_in[...], fac_hi[...], fac_lo[...], NT)
        solved[...] = dot_split(resid[...], inv_hi[...], inv_lo[...], NN)
        s_out[0] = solved[...].astype(s_out.dtype)
        send_s(0, 0, 3, 2).start()
        prepare_back()
        solved[...] -= take_v(3, 2)
        v_out[...] = apply(
            solved[...].astype(w_out.dtype), step_t_hi[...], step_t_lo[...], NN
        ).astype(v_out.dtype)
        send_v(1, 0).start()
        finish(2, solved[...])

    @pl.when(role(3, 2))
    def _():
        whole = prepare_back()
        step_hi[...], step_lo[...] = split(whole.T)
        gather_fit()
        take_u(0)
        take_u(1)
        resid[...] = dot_split(resid[...], inv_hi[...], inv_lo[...], NN)
        wait_s()
        solved[...] = resid[...] - apply(s_in[...], step_hi[...], step_lo[...], NN)
        back = apply(solved[...].astype(w_out.dtype), step_t_hi[...], step_t_lo[...], NN)
        v_out[...] = back.astype(v_out.dtype)
        send_v(2, 1).start()
        w_out[1] = (s_in[...].astype(F32) - back).astype(w_out.dtype)
        send_w(2, 1, 2, 0).start()
        coef = dot_split(solved[...], inv_t_hi[...], inv_t_lo[...], NN)
        w_out[0] = coef.astype(w_out.dtype)
        send_w(0, 0, 3, 0).start()
        send_w(1, 0, 3, 1).start()
        for c in range(members):
            rounded[c] = coef[:, c * height:(c + 1) * height].astype(BF16)
        spread_rounded(3, True)

    @pl.when(jnp.logical_and(later, jnp.logical_not(lead_home)))
    def _():
        remote(rounded.at[0], rounded.at[0], round_send.at[0, 0], round_recv, row, col).wait_recv()

    for c in range(members):
        @pl.when(jnp.logical_and(first, member == c))
        def _():
            right = pl.ds(c * height, block - c * height)
            remote(
                last_out.at[:, right], last_in.at[:, right], last_send.at[c, 0], last_recv, row, col
            ).wait_recv()
            rounded[c] = apply(last_in[:, right], inv_hi[own, right], inv_lo[own, right], NT).astype(BF16)

    mine_rounded = rounded[member]

    def product(target):
        span = pl.ds(pl.multiple_of(target * share, TILE), share)
        return lax.dot_general(mine_rounded, masked[:, span], NN, preferred_element_type=F32)

    def part_copy(i):
        target = lax.rem(row + n_aux - i, n_aux)
        return target, remote(
            part_out.at[target], part_in.at[row], part_send.at[target], part_recv.at[row], target, col
        )

    def give(i, carry):
        target, copy = part_copy(i)
        part_out[target] = product(target).astype(BF16)
        copy.start()
        return carry

    lax.fori_loop(1, n_aux, give, 0)
    total = product(row)

    def take(i, total):
        source = lax.rem(row + i, n_aux)
        remote(part_out.at[0], part_in.at[source], part_send.at[0], part_recv.at[source], row, col).wait_recv()
        return total + part_in[source].astype(F32)

    out[...] = lax.fori_loop(1, n_aux, take, total)

    for c in range(lead):
        @pl.when(member == c)
        def _():
            @pl.when(below)
            def _():
                move_fac(c).wait_send()

            @pl.when(with_inv)
            def _():
                move_inv(c).wait_send()

    for c in range(members):
        @pl.when(jnp.logical_and(first, member == c))
        def _():
            for i in range(len(p_targets)):
                send_p(c, i).wait_send()

    @pl.when(sends_fit)
    def _():
        send_fit.wait_send()

    @pl.when(role(1, 0))
    def _():
        send_s(2, 0, 3, 0).wait_send()
        send_s(0, 1, 2, 1).wait_send()
        send_s(1, 1, 3, 1).wait_send()
        for z in range(n_pair):
            for c in range(members):
                last_copy(c, z).wait_send()
        spread_rounded(1, False)

    @pl.when(role(2, 0))
    def _():
        send_u(2).wait_send()
        send_v(1, 0).wait_send()

    @pl.when(jnp.logical_or(role(3, 0), role(3, 1)))
    def _():
        send_u(3).wait_send()
        send_v(1, 0).wait_send()

    @pl.when(role(2, 1))
    def _():
        send_s(0, 0, 3, 2).wait_send()
        send_v(1, 0).wait_send()
        spread_rounded(2, False)

    @pl.when(role(3, 2))
    def _():
        send_v(2, 1).wait_send()
        send_w(2, 1, 2, 0).wait_send()
        send_w(0, 0, 3, 0).wait_send()
        send_w(1, 0, 3, 1).wait_send()
        spread_rounded(3, False)

    def sent(i, carry):
        part_copy(i)[1].wait_send()
        return carry

    lax.fori_loop(1, n_aux, sent, 0)


def shards(integrals, densities, screen, factor, diag_inv):
    n_aux, n_pair = lax.axis_size("aux"), lax.axis_size("pair")
    height, width = integrals.shape
    breadth, block = factor.shape[1], diag_inv.shape[1]
    count = densities.shape[0]
    members, pieces = block // height, breadth // height
    share = width // n_aux
    vmem, dma = pltpu.VMEM, pltpu.SemaphoreType.DMA

    def rows(*lead):
        return vmem(lead + (count, height), F32)

    def whole(*lead, kind=F32):
        return vmem(lead + (count, block), kind)

    weights = 2 * block * block * 4 + 10 * block * block * 2
    fits = weights + integrals.size * 2 <= VMEM_ROOM
    if breadth == block and members == 2 and n_pair == SOLVE_BLOCKS and fits:
        body = lead_kernel
        screen_space = pl.ANY
        scratch = [
            pltpu.SMEM(screen.shape, screen.dtype), vmem((height, width), BF16), vmem((count, width), BF16),
            vmem((block, block), F32), vmem((block, block), F32),
            *[vmem((block, block), BF16) for _ in range(10)],
            rows(), rows(n_pair, members), whole(kind=P_KIND), whole(n_pair, members, kind=P_KIND),
            whole(kind=U_KIND), whole(n_pair, kind=U_KIND), whole(2, kind=S_KIND), whole(kind=S_KIND),
            whole(2, kind=BF16), whole(kind=BF16), whole(kind=V_KIND), whole(SOLVE_BLOCKS, n_pair, kind=V_KIND),
            whole(), whole(), whole(), vmem((members, count, height), BF16),
            whole(kind=L_KIND), whole(kind=L_KIND),
            vmem((n_aux, count, share), BF16), vmem((n_aux, count, share), BF16),
            dma((width // STREAM,)), dma((4,)),
            dma, dma((members,)), dma, dma((members,)),
            dma, dma((n_pair, members)), dma((2,)), dma((n_pair, members)), dma, dma((n_pair,)),
            dma((3,)), dma, dma((3,)), dma, dma, dma((SOLVE_BLOCKS, n_pair)),
            dma((members, n_pair)), dma, dma((members, n_pair)), dma,
            dma((n_aux,)), dma((n_aux,)),
        ]
    else:
        body = spread_kernel
        screen_space = pltpu.SMEM
        scratch = [
            vmem((height, width), BF16), vmem((count, width), BF16),
            vmem((height, breadth), F32), vmem((height, block), F32),
            vmem((height, breadth), BF16), vmem((height, breadth), BF16),
            vmem((height, block), BF16), vmem((height, block), BF16),
            rows(), rows(n_pair), rows(), rows(n_pair),
            rows(members), rows(members, pieces), rows(pieces), rows(members, members),
            rows(members), rows(), rows(pieces), rows(n_aux, members),
            vmem((n_aux, count, share), BF16), vmem((n_aux, count, share), BF16),
            dma((width // STREAM,)), dma((3,)),
            dma, dma((n_pair,)), dma, dma((n_pair,)),
            dma((members, n_aux)), dma((members, pieces)),
            dma((members, members)), dma((members, members)),
            dma((n_pair,)), dma, dma((pieces, members)), dma((n_aux, members)),
            dma((n_aux,)), dma((n_aux,)),
        ]
    return pl.pallas_call(
        functools.partial(body, n_aux, n_pair),
        out_shape=jax.ShapeDtypeStruct((count, share), F32),
        in_specs=[
            pl.BlockSpec(memory_space=pl.ANY),
            pl.BlockSpec(memory_space=pl.ANY),
            pl.BlockSpec(memory_space=screen_space),
            pl.BlockSpec(memory_space=pl.ANY),
            pl.BlockSpec(memory_space=pl.ANY),
        ],
        out_specs=pl.BlockSpec(memory_space=pltpu.VMEM),
        scratch_shapes=scratch,
        compiler_params=pltpu.CompilerParams(
            collective_id=0, has_side_effects=True, vmem_limit_bytes=60 * 2**20
        ),
    )(integrals, densities, screen, factor, diag_inv)


def solution(mesh):
    in_specs = (
        P("aux", "pair"),
        P(None, "pair"),
        P("aux", "pair"),
        P("aux", "pair"),
        P("aux", None),
    )
    out_specs = P(None, ("pair", "aux"))
    return jax.shard_map(shards, mesh=mesh, in_specs=in_specs, out_specs=out_specs, check_vma=False)
```

```python
import functools

import jax
import jax.numpy as jnp
from jax import lax
from jax.experimental import pallas as pl
from jax.experimental.pallas import tpu as pltpu
from jax.sharding import PartitionSpec as P

TILE = 128
SOLVE_BLOCKS = 4
STREAM = 1024
LEAD_STREAM = 2048
VMEM_ROOM = 48 * 2**20
MESH = pl.DeviceIdType.MESH
NN = (((1,), (0,)), ((), ()))
NT = (((1,), (1,)), ((), ()))
F32 = jnp.float32
BF16 = jnp.bfloat16
P_KIND, S_KIND, V_KIND, L_KIND = BF16, BF16, BF16, BF16
VMEM_LIMIT = 56400000


def split(values):
    high = values.astype(BF16)
    return high, (values - high.astype(F32)).astype(BF16)


def dot_split(values, high, low, dims):
    top, rest = split(values)
    rows = values.shape[0]
    both = lax.dot_general(
        jnp.concatenate([top, rest], 0), high, dims, preferred_element_type=F32
    )
    minor = lax.dot_general(top, low, dims, preferred_element_type=F32)
    return both[:rows] + (both[rows:] + minor)


def spread_kernel(
    n_aux, n_pair,
    integrals, densities, screen, factor, diag_inv, out,
    masked, dens, fac, inv, fac_hi, fac_lo, inv_hi, inv_lo,
    fit_out, fit_in, u_out, u_in, s_out, s_in, s_sum, own_in, resid, coef, v_out, v_in,
    part_out, part_in,
    load_sem, small_sem,
    fit_send, fit_recv, u_send, u_recv, s_send, s_recv, own_send, own_recv,
    coef_send, coef_recv, v_send, v_recv, part_send, part_recv,
):
    height, width = masked.shape
    breadth = fac.shape[1]
    block = inv.shape[1]
    members = block // height
    group = block // breadth
    pieces = breadth // height
    share = width // n_aux
    chunks = width // STREAM

    row = lax.axis_index("aux")
    col = lax.axis_index("pair")
    mine = row // members
    member = lax.rem(row, members)
    column_block = col // group
    column_part = lax.rem(col, group)

    def home_of(k):
        return jnp.maximum(k - 1, 0) * group

    home = home_of(mine)
    is_home = col == home
    below = column_block < mine

    def remote(src, dst, send, recv, aux, pair):
        return pltpu.make_async_remote_copy(
            src_ref=src, dst_ref=dst, send_sem=send, recv_sem=recv,
            device_id={"aux": aux, "pair": pair}, device_id_type=MESH,
        )

    def load(c):
        at = pl.ds(pl.multiple_of(c * STREAM, STREAM), STREAM)
        return pltpu.make_async_copy(integrals.at[:, at], masked.at[:, at], load_sem.at[c])

    load_dens = pltpu.make_async_copy(densities, dens, small_sem.at[0])
    load_fac = pltpu.make_async_copy(factor, fac, small_sem.at[1])
    load_inv = pltpu.make_async_copy(diag_inv, inv, small_sem.at[2])
    load_dens.start()
    for c in range(chunks):
        load(c).start()
    load_inv.start()

    @pl.when(below)
    def _():
        load_fac.start()

    barrier = pltpu.get_barrier_semaphore()
    everyone = n_aux * n_pair
    me = row * n_pair + col

    def greet(i, carry):
        other = lax.rem(me + i, everyone)
        pl.semaphore_signal(
            barrier, inc=1,
            device_id={"aux": other // n_pair, "pair": lax.rem(other, n_pair)},
            device_id_type=MESH,
        )
        return carry

    lax.fori_loop(1, everyone, greet, 0)
    load_dens.wait()

    def fit_step(c, total):
        load(c).wait()
        base = pl.multiple_of(c * STREAM, STREAM)
        for r in range(height // TILE):
            for t in range(STREAM // TILE):
                flag = screen[r, c * (STREAM // TILE) + t].astype(F32)
                at = (pl.ds(r * TILE, TILE), pl.ds(pl.multiple_of(base + t * TILE, TILE), TILE))
                masked[at] = masked[at] * jnp.full((TILE, TILE), flag, F32).astype(BF16)
        span = pl.ds(base, STREAM)
        return total + lax.dot_general(
            dens[:, span], masked[:, span], NT, preferred_element_type=F32
        )

    fitted = lax.fori_loop(0, chunks, fit_step, jnp.zeros((dens.shape[0], height), F32))
    fit_out[...] = fitted
    pl.semaphore_wait(barrier, everyone - 1)

    send_fit = remote(fit_out, fit_in.at[col], fit_send, fit_recv.at[col], row, home)

    @pl.when(jnp.logical_not(is_home))
    def _():
        send_fit.start()

    load_inv.wait()
    high, low = split(inv[...])
    inv_hi[...] = high
    inv_lo[...] = low

    @pl.when(below)
    def _():
        load_fac.wait()
        high, low = split(fac[...])
        fac_hi[...] = high
        fac_lo[...] = low

    @pl.when(below)
    def _():
        for x in range(pieces):
            whole_x = column_part * pieces + x
            for c in range(members):
                @pl.when(whole_x >= c)
                def _():
                    remote(s_out.at[0], s_in.at[c, x], s_send.at[0, 0], s_recv.at[c, x], row, col).wait_recv()
                    if c == 0:
                        s_sum[x] = s_in[c, x]
                    else:
                        s_sum[x] += s_in[c, x]
        known = jnp.concatenate([s_sum[x] for x in range(pieces)], 1)
        u_out[...] = dot_split(known, fac_hi[...], fac_lo[...], NT)

        @pl.when(jnp.logical_not(is_home))
        def _():
            remote(u_out, u_in.at[col], u_send, u_recv.at[col], row, home).start()

    def send_solved(x, start):
        part, piece = x // pieces, x % pieces

        def later(d, carry):
            copy = remote(
                s_out.at[x], s_in.at[member, piece], s_send.at[x, d],
                s_recv.at[member, piece], d, mine * group + part,
            )
            copy.start() if start else copy.wait_send()
            return carry

        lax.fori_loop((mine + 1) * members, n_aux, later, 0)
        for i in range(1, members):
            other = lax.rem(member + i, members)

            @pl.when(other <= x)
            def _():
                copy = remote(
                    s_out.at[x], own_in.at[member, x], own_send.at[x, i],
                    own_recv.at[member, x], mine * members + other, home,
                )
                copy.start() if start else copy.wait_send()

    @pl.when(is_home)
    def _():
        fit_total = fit_out
        for p in range(n_pair):
            @pl.when(p != home)
            def _():
                remote(fit_out, fit_in.at[p], fit_send, fit_recv.at[p], row, col).wait_recv()
                fit_total[...] += fit_in[p]
        for p in range(n_pair):
            @pl.when(jnp.logical_and(p // group < mine, p != home))
            def _():
                remote(u_out, u_in.at[p], u_send, u_recv.at[p], row, col).wait_recv()
                fit_total[...] -= u_in[p]

        @pl.when(below)
        def _():
            fit_total[...] -= u_out[...]

        for x in range(members):
            @pl.when(x >= member)
            def _():
                at = pl.ds(x * height, height)
                s_out[x] = dot_split(fit_total[...], inv_hi[:, at], inv_lo[:, at], NN)
                send_solved(x, True)

        for x in range(members):
            @pl.when(x >= member)
            def _():
                resid[x] = s_out[x]
                for i in range(1, members):
                    other = lax.rem(member + i, members)

                    @pl.when(other <= x)
                    def _():
                        remote(s_out.at[0], own_in.at[other, x], own_send.at[0, 0], own_recv.at[other, x], row, col).wait_recv()
                        resid[x] += own_in[other, x]

        def subtract(i, carry):
            source = n_aux - 1 - i
            for x in range(members):
                @pl.when(x >= member)
                def _():
                    remote(v_out.at[0], v_in.at[source, x], v_send.at[0, 0], v_recv.at[source, x], row, col).wait_recv()
                    resid[x] -= v_in[source, x]
            return carry

        lax.fori_loop(0, n_aux - (mine + 1) * members, subtract, 0)
        for x in reversed(range(members)):
            @pl.when(x >= member)
            def _():
                at = pl.ds(x * height, height)
                term = dot_split(resid[x], inv_hi[:, at], inv_lo[:, at], NT)
                if x == members - 1:
                    coef[...] = term
                else:
                    coef[...] += term

        for i in range(1, n_pair):
            remote(coef, coef, coef_send.at[i], coef_recv, row, lax.rem(col + i, n_pair)).start()

    @pl.when(jnp.logical_not(is_home))
    def _():
        remote(coef, coef, coef_send.at[0], coef_recv, row, col).wait_recv()

    def send_v(x, start):
        whole_x = column_part * pieces + x
        for c in range(members):
            @pl.when(c <= whole_x)
            def _():
                copy = remote(
                    v_out.at[x], v_in.at[row, whole_x], v_send.at[x, c],
                    v_recv.at[row, whole_x], column_block * members + c, home_of(column_block),
                )
                copy.start() if start else copy.wait_send()

    @pl.when(below)
    def _():
        for x in range(pieces):
            at = pl.ds(x * height, height)
            v_out[x] = dot_split(coef[...], fac_hi[:, at], fac_lo[:, at], NN)
            send_v(x, True)

    rounded = coef[...].astype(BF16)

    def product(target):
        span = pl.ds(pl.multiple_of(target * share, TILE), share)
        return lax.dot_general(rounded, masked[:, span], NN, preferred_element_type=F32)

    def part_copy(i):
        target = lax.rem(row + i, n_aux)
        return target, remote(
            part_out.at[target], part_in.at[row], part_send.at[target], part_recv.at[row], target, col
        )

    def give(i, carry):
        target, copy = part_copy(i)
        part_out[target] = product(target).astype(BF16)
        copy.start()
        return carry

    lax.fori_loop(1, n_aux, give, 0)
    total = product(row)

    def take(i, total):
        source = lax.rem(row + n_aux - i, n_aux)
        remote(part_out.at[0], part_in.at[source], part_send.at[0], part_recv.at[source], row, col).wait_recv()
        return total + part_in[source].astype(F32)

    out[...] = lax.fori_loop(1, n_aux, take, total)

    @pl.when(jnp.logical_not(is_home))
    def _():
        send_fit.wait_send()

        @pl.when(below)
        def _():
            remote(u_out, u_in.at[col], u_send, u_recv.at[col], row, home).wait_send()

    @pl.when(is_home)
    def _():
        for x in range(members):
            @pl.when(x >= member)
            def _():
                send_solved(x, False)
        for i in range(1, n_pair):
            remote(coef, coef, coef_send.at[i], coef_recv, row, lax.rem(col + i, n_pair)).wait_send()

    @pl.when(below)
    def _():
        for x in range(pieces):
            send_v(x, False)

    def sent(i, carry):
        part_copy(i)[1].wait_send()
        return carry

    lax.fori_loop(1, n_aux, sent, 0)


def dot_two(values, high, low, dims):
    return lax.dot_general(values, high, dims, preferred_element_type=F32) + lax.dot_general(
        values, low, dims, preferred_element_type=F32
    )


def apply(values, high, low, dims):
    return (dot_two if values.dtype == BF16 else dot_split)(values, high, low, dims)


def lead_kernel(
    n_aux, n_pair,
    integrals, densities, screen, factor, diag_inv, out,
    flags, masked, dens, fac, inv, fac_hi, fac_lo, inv_hi, inv_lo, inv_t_hi, inv_t_lo,
    step_hi, step_lo, step_t_hi, step_t_lo,
    fit_out, fit_in, p_out, p_in, u_out, u_in, s_out, s_in, t_out, t_in, w_out, w_in, v_out, v_in, y_out, y_in,
    resid, solved, start, rounded, last_out, last_in, part_out, part_in,
    load_sem, small_sem, fac_send, fac_recv, inv_send, inv_recv,
    fit_send, fit_recv, p_send, p_recv, u_send, u_recv, s_send, s_recv, t_send, t_recv, w_send, w_recv,
    v_send, v_recv, y_send, y_recv, round_send, round_recv, last_send, last_recv, part_send, part_recv,
):
    height, width = masked.shape
    block = inv.shape[1]
    count = dens.shape[0]
    members = block // height
    share = width // n_aux
    chunks = width // LEAD_STREAM
    strips = height // TILE

    row = lax.axis_index("aux")
    col = lax.axis_index("pair")
    mine = row // members
    member = lax.rem(row, members)
    lead = members - 1
    lead_row = mine * members + lead
    is_lead = member == lead
    first = mine == 0
    later = mine > 0
    home = jnp.maximum(mine - 1, 0)
    at_home = jnp.logical_and(later, col == home)
    below = col < mine

    def chip(k, z):
        return jnp.logical_and(mine == k, col == z)

    def role(k, z):
        return jnp.logical_and(is_lead, chip(k, z))

    lead_home = jnp.logical_and(is_lead, at_home)
    lead_below = jnp.logical_and(is_lead, below)

    def remote(src, dst, send, recv, aux, pair):
        return pltpu.make_async_remote_copy(
            src_ref=src, dst_ref=dst, send_sem=send, recv_sem=recv,
            device_id={"aux": aux, "pair": pair}, device_id_type=MESH,
        )

    def to_lead(src, dst, send, recv, k, z):
        return remote(src, dst, send, recv, k * members + lead, z)

    def load(c):
        at = pl.ds(pl.multiple_of(c * LEAD_STREAM, LEAD_STREAM), LEAD_STREAM)
        return pltpu.make_async_copy(integrals.at[:, at], masked.at[:, at], load_sem.at[c])

    own = pl.ds(lead * height, height)
    load_dens = pltpu.make_async_copy(densities, dens, small_sem.at[0])
    load_fac = pltpu.make_async_copy(factor, fac.at[own], small_sem.at[1])
    load_inv = pltpu.make_async_copy(diag_inv, inv.at[own], small_sem.at[2])
    load_flags = pltpu.make_async_copy(screen, flags, small_sem.at[3])

    def move_fac(c):
        return remote(factor, fac.at[pl.ds(c * height, height)], fac_send, fac_recv.at[c], lead_row, col)

    def move_inv(c):
        right = pl.ds(c * height, block - c * height)
        return remote(
            diag_inv.at[:, right], inv.at[pl.ds(c * height, height), right],
            inv_send, inv_recv.at[c], lead_row, col,
        )

    def load_start(c):
        right = pl.ds(c * height, block - c * height)
        return pltpu.make_async_copy(diag_inv.at[:, right], inv.at[own, right], small_sem.at[2])

    load_flags.start()
    load_dens.start()
    for c in range(chunks):
        load(c).start()
    for c in range(members):
        @pl.when(jnp.logical_and(first, member == c))
        def _():
            load_start(c).start()


    @pl.when(lead_below)
    def _():
        load_fac.start()
        load_inv.start()

    barrier = pltpu.get_barrier_semaphore()

    def greet(k, c, z):
        pl.semaphore_signal(
            barrier, inc=1, device_id={"aux": k * members + c, "pair": z}, device_id_type=MESH
        )

    c_one, c_two, c_three = role(1, 0), role(2, 1), role(3, 2)
    lead_aside = jnp.logical_and(lead_below, jnp.logical_not(at_home))

    @pl.when(jnp.logical_or(c_one, role(2, 0)))
    def _():
        for c in range(members):
            for z in range(n_pair):
                greet(0, c, z)

    @pl.when(lead_home)
    def _():
        for c in range(members):
            for i in range(n_pair):
                if c != lead or i:
                    greet(mine, c, lax.rem(col + i, n_pair))

    @pl.when(lead_aside)
    def _():
        for c in range(lead):
            greet(mine, c, col)

    @pl.when(jnp.logical_or(c_two, jnp.logical_and(lead_aside, mine == 3)))
    def _():
        greet(1, lead, 0)

    @pl.when(c_three)
    def _():
        greet(2, lead, 1)

    gives = jnp.logical_and(jnp.logical_not(is_lead), below)
    greeted = (
        jnp.where(first, 2, 0)
        + jnp.where(jnp.logical_and(later, jnp.logical_not(lead_home)), 1, 0)
        + jnp.where(jnp.logical_and(gives, jnp.logical_not(at_home)), 1, 0)
        + jnp.where(c_one, 3, 0)
        + jnp.where(c_two, 1, 0)
    )

    @pl.when(gives)
    def _():
        pl.semaphore_wait(barrier, greeted)

    for c in range(lead):
        @pl.when(jnp.logical_and(gives, member == c))
        def _():
            move_fac(c).start()
            move_inv(c).start()

    load_flags.wait()
    load_dens.wait()

    def flag_of(r, t):
        return flags[r, t].astype(F32)

    def fit_step(c, sums):
        base = pl.multiple_of(c * LEAD_STREAM, LEAD_STREAM)
        kept = []
        for r in range(strips):
            tiles = []
            for t in range(LEAD_STREAM // TILE):
                at = pl.ds(pl.multiple_of(base + t * TILE, TILE), TILE)
                flag = flag_of(r, c * (LEAD_STREAM // TILE) + t)
                tiles.append(dens[:, at] * jnp.full((count, TILE), flag, F32).astype(BF16))
            kept.append(jnp.concatenate(tiles, 1))
        load(c).wait()
        return tuple(
            sums[r] + lax.dot_general(
                kept[r], masked[pl.ds(r * TILE, TILE), pl.ds(base, LEAD_STREAM)], NT,
                preferred_element_type=F32,
            )
            for r in range(strips)
        )

    sums = lax.fori_loop(
        0, chunks - 1, fit_step, tuple(jnp.zeros((count, TILE), F32) for _ in range(strips))
    )
    for c in range(members):
        @pl.when(jnp.logical_and(first, member == c))
        def _():
            right = pl.ds(c * height, block - c * height)
            load_start(c).wait()
            inv_hi[own, right], inv_lo[own, right] = split(inv[own, right])

    sums = fit_step(chunks - 1, sums)
    for r in range(strips):
        fit_out[:, pl.ds(r * TILE, TILE)] = sums[r]

    p_targets = ((1, 0), (2, 0))

    def send_p(c, i):
        right = pl.ds(c * height, block - c * height)
        return to_lead(
            p_out.at[:, right], p_in.at[col, c, :, right], p_send.at[i], p_recv.at[col, c], *p_targets[i]
        )

    for c in range(members):
        @pl.when(jnp.logical_and(first, member == c))
        def _():
            right = pl.ds(c * height, block - c * height)
            p_out[:, right] = dot_split(
                fit_out[...], inv_hi[own, right], inv_lo[own, right], NN
            ).astype(p_out.dtype)

    @pl.when(jnp.logical_not(jnp.logical_or(gives, c_three)))
    def _():
        pl.semaphore_wait(barrier, greeted)


    for c in range(members):
        @pl.when(jnp.logical_and(first, member == c))
        def _():
            for i in range(len(p_targets)):
                send_p(c, i).start()

    send_fit = remote(
        fit_out, fit_in.at[col, member], fit_send, fit_recv.at[col, member], lead_row, home
    )
    sends_fit = jnp.logical_and(later, jnp.logical_not(lead_home))

    @pl.when(sends_fit)
    def _():
        send_fit.start()

    def mask_step(c, carry):
        base = pl.multiple_of(c * LEAD_STREAM, LEAD_STREAM)
        for r in range(strips):
            for t in range(LEAD_STREAM // TILE):
                flag = flag_of(r, c * (LEAD_STREAM // TILE) + t)
                at = (pl.ds(r * TILE, TILE), pl.ds(pl.multiple_of(base + t * TILE, TILE), TILE))
                masked[at] = masked[at] * jnp.full((TILE, TILE), flag, F32).astype(BF16)
        return carry

    lax.fori_loop(0, chunks, mask_step, 0)

    @pl.when(lead_below)
    def _():
        load_fac.wait()
        for c in range(lead):
            move_fac(c).wait_recv()
        fac_hi[...], fac_lo[...] = split(fac[...])
        load_inv.wait()
        for c in range(lead):
            move_inv(c).wait_recv()
        inv_hi[...], inv_lo[...] = split(inv[...])

    def prepare_back():
        inv_t_hi[...], inv_t_lo[...] = split(inv[...].T)
        whole = lax.dot_general(inv_t_hi[...], fac_hi[...], NN, preferred_element_type=F32)
        whole += lax.dot_general(inv_t_lo[...], fac_hi[...], NN, preferred_element_type=F32)
        whole += lax.dot_general(inv_t_hi[...], fac_lo[...], NN, preferred_element_type=F32)
        step_t_hi[...], step_t_lo[...] = split(whole)
        return whole

    def prepare_ahead():
        whole = prepare_back()
        step_hi[...], step_lo[...] = split(whole.T)

    def turn_fac():
        step_hi[...], step_lo[...] = split(fac[...].T)

    def gather_fit():
        resid[:, own] = fit_out[...]
        for c in range(lead):
            for p in range(n_pair):
                @pl.when(p == home)
                def _():
                    remote(fit_out, fit_in.at[p, c], fit_send, fit_recv.at[p, c], row, col).wait_recv()
                    resid[:, pl.ds(c * height, height)] = fit_in[p, c]
        for p in range(n_pair):
            for c in range(members):
                @pl.when(p != home)
                def _():
                    remote(fit_out, fit_in.at[p, c], fit_send, fit_recv.at[p, c], row, col).wait_recv()
                    resid[:, pl.ds(c * height, height)] += fit_in[p, c]

    def gather_start():
        for p in range(n_pair):
            for c in range(members):
                right = pl.ds(c * height, block - c * height)
                remote(
                    p_out.at[:, right], p_in.at[p, c, :, right], p_send.at[0], p_recv.at[p, c], row, col
                ).wait_recv()
        for c in range(members):
            at = pl.ds(c * height, height)
            sum_p = p_in[0, 0, :, at].astype(F32)
            for p in range(n_pair):
                for d in range(c + 1):
                    if p or d:
                        sum_p += p_in[p, d, :, at].astype(F32)
            start[:, at] = sum_p

    def send_s(k, z):
        return to_lead(s_out, s_in, s_send, s_recv, k, z)

    def send_t(slot, k, z):
        return to_lead(t_out.at[slot], t_in, t_send.at[slot], t_recv, k, z)

    def send_u(k):
        return to_lead(u_out, u_in.at[col], u_send, u_recv.at[col], k, k - 1)

    def send_v(k, z):
        return to_lead(v_out, v_in, v_send, v_recv, k, z)

    def send_y():
        return to_lead(y_out, y_in.at[mine, col], y_send, y_recv.at[mine, col], 1, 0)

    def send_w(i, slot, k, z):
        return to_lead(w_out.at[slot], w_in, w_send.at[i], w_recv, k, z)

    def wait_s():
        send_s(0, 0).wait_recv()

    def take_u(p):
        remote(u_out, u_in.at[p], u_send, u_recv.at[p], row, col).wait_recv()
        resid[...] -= u_in[p].astype(F32)

    def take_v():
        remote(v_out, v_in, v_send, v_recv, row, col).wait_recv()
        return v_in[...].astype(F32)

    def take_y(k, z):
        remote(y_out, y_in.at[k, z], y_send, y_recv.at[k, z], row, col).wait_recv()
        return y_in[k, z]

    def wait_w():
        send_w(0, 0, 0, 0).wait_recv()

    def round_copy(k, c, i, z):
        return remote(
            rounded.at[c], rounded.at[c], round_send.at[c, i], round_recv, k * members + c, lax.rem(z + i, n_pair)
        )

    def spread_rounded(k, go):
        for i in reversed(range(n_pair)):
            for c in range(members):
                if c != lead or i:
                    copy = round_copy(k, c, i, k - 1)
                    copy.start() if go else copy.wait_send()

    def finish(k, values):
        coef = dot_split(values, inv_t_hi[...], inv_t_lo[...], NN)
        for c in range(members):
            rounded[c] = coef[:, c * height:(c + 1) * height].astype(BF16)
        spread_rounded(k, True)

    def last_copy(c, z):
        right = pl.ds(c * height, block - c * height)
        return remote(
            last_out.at[:, right], last_in.at[:, right], last_send.at[c, z], last_recv, c, z
        )

    @pl.when(role(1, 0))
    def _():
        turn_fac()
        gather_fit()
        gather_start()
        t_out[0] = start[...]
        send_t(0, 3, 0).start()
        resid[...] -= dot_split(start[...], step_hi[...], step_lo[...], NN)
        solved[...] = dot_split(resid[...], inv_hi[...], inv_lo[...], NN)
        s_out[...] = solved[...].astype(s_out.dtype)
        t_out[1] = solved[...]
        send_s(2, 1).start()
        send_t(1, 3, 1).start()
        prepare_back()
        solved[...] -= take_y(3, 1)
        start[...] -= take_y(3, 0)
        solved[...] -= take_v()
        back = dot_split(solved[...], step_t_hi[...], step_t_lo[...], NN)
        last_out[...] = (start[...] - take_y(2, 0) - back).astype(last_out.dtype)
        for z in reversed(range(n_pair)):
            for c in range(members):
                last_copy(c, z).start()
        finish(1, solved[...])

    @pl.when(role(2, 0))
    def _():
        turn_fac()
        gather_start()
        u_out[...] = dot_split(start[...], step_hi[...], step_lo[...], NN)
        send_u(2).start()
        prepare_back()
        wait_w()
        y_out[...] = dot_split(w_in[...], step_t_hi[...], step_t_lo[...], NN)
        send_y().start()

    @pl.when(jnp.logical_or(role(3, 0), role(3, 1)))
    def _():
        prepare_ahead()
        send_t(0, 0, 0).wait_recv()
        u_out[...] = dot_split(t_in[...], step_hi[...], step_lo[...], NN)
        send_u(3).start()
        wait_w()
        y_out[...] = dot_split(w_in[...], step_t_hi[...], step_t_lo[...], NN)
        send_y().start()

    @pl.when(role(2, 1))
    def _():
        prepare_ahead()
        gather_fit()
        take_u(0)
        resid[...] = dot_split(resid[...], inv_hi[...], inv_lo[...], NN)
        wait_s()
        solved[...] = resid[...] - apply(s_in[...], step_hi[...], step_lo[...], NN)
        s_out[...] = solved[...].astype(s_out.dtype)
        send_s(3, 2).start()
        solved[...] -= take_v()
        v_out[...] = dot_split(solved[...], step_t_hi[...], step_t_lo[...], NN).astype(v_out.dtype)
        send_v(1, 0).start()
        finish(2, solved[...])

    @pl.when(role(3, 2))
    def _():
        prepare_ahead()
        gather_fit()
        resid[...] = dot_split(resid[...], inv_hi[...], inv_lo[...], NN)
        take_u(0)
        take_u(1)
        wait_s()
        solved[...] = resid[...] - apply(s_in[...], step_hi[...], step_lo[...], NN)
        w_out[0] = solved[...]
        send_w(0, 0, 3, 1).start()
        send_w(1, 0, 3, 0).start()
        back = dot_split(solved[...], step_t_hi[...], step_t_lo[...], NN)
        v_out[...] = back.astype(v_out.dtype)
        send_v(2, 1).start()
        w_out[1] = s_in[...].astype(F32) - back
        send_w(2, 1, 2, 0).start()
        coef = dot_split(solved[...], inv_t_hi[...], inv_t_lo[...], NN)
        for c in range(members):
            rounded[c] = coef[:, c * height:(c + 1) * height].astype(BF16)
        spread_rounded(3, True)

    @pl.when(jnp.logical_and(later, jnp.logical_not(lead_home)))
    def _():
        remote(rounded.at[0], rounded.at[0], round_send.at[0, 0], round_recv, row, col).wait_recv()

    for c in range(members):
        @pl.when(jnp.logical_and(first, member == c))
        def _():
            right = pl.ds(c * height, block - c * height)
            remote(
                last_out.at[:, right], last_in.at[:, right], last_send.at[c, 0], last_recv, row, col
            ).wait_recv()
            rounded[c] = apply(last_in[:, right], inv_hi[own, right], inv_lo[own, right], NT).astype(BF16)

    mine_rounded = rounded[member]

    span = members * share

    def product(group):
        at = pl.ds(pl.multiple_of(group * span, TILE), span)
        return lax.dot_general(mine_rounded, masked[:, at], NN, preferred_element_type=F32)

    def flipped(mask):
        group, unit = 0, 1
        while unit * members < n_aux:
            digit = lax.rem(mine // unit, 2)
            group = group + unit * (1 - digit if mask & unit else digit)
            unit *= 2
        return group

    order = sorted(range(1, n_aux // members), key=lambda m: -bin(m).count("1"))
    partner = mine * members + 1 - member

    def part_copy(target):
        return remote(
            part_out.at[target], part_in.at[row], part_send.at[target], part_recv.at[row], target, col
        )

    for mask in order:
        group = flipped(mask)
        values = product(group)
        for c in range(members):
            part_out[group * members + c] = values[:, c * share:(c + 1) * share].astype(BF16)
            part_copy(group * members + c).start()

    values = product(mine)
    halves = values[:, :share], values[:, share:]
    part_out[partner] = jnp.where(member == 0, halves[1], halves[0]).astype(BF16)
    part_copy(partner).start()
    total = jnp.where(member == 0, halves[0], halves[1])

    def take(source):
        remote(part_out.at[0], part_in.at[source], part_send.at[0], part_recv.at[source], row, col).wait_recv()
        return part_in[source].astype(F32)

    total += take(partner)
    for mask in reversed(order):
        for c in range(members):
            total += take(flipped(mask) * members + c)

    out[...] = total

    for c in range(lead):
        @pl.when(member == c)
        def _():
            @pl.when(below)
            def _():
                move_fac(c).wait_send()
                move_inv(c).wait_send()

    for c in range(members):
        @pl.when(jnp.logical_and(first, member == c))
        def _():
            for i in range(len(p_targets)):
                send_p(c, i).wait_send()

    @pl.when(sends_fit)
    def _():
        send_fit.wait_send()

    @pl.when(role(1, 0))
    def _():
        send_t(0, 3, 0).wait_send()
        send_s(2, 1).wait_send()
        send_t(1, 3, 1).wait_send()
        for z in range(n_pair):
            for c in range(members):
                last_copy(c, z).wait_send()
        spread_rounded(1, False)

    @pl.when(role(2, 0))
    def _():
        send_u(2).wait_send()
        send_y().wait_send()

    @pl.when(jnp.logical_or(role(3, 0), role(3, 1)))
    def _():
        send_u(3).wait_send()
        send_y().wait_send()

    @pl.when(role(2, 1))
    def _():
        send_s(3, 2).wait_send()
        send_v(1, 0).wait_send()
        spread_rounded(2, False)

    @pl.when(role(3, 2))
    def _():
        send_v(2, 1).wait_send()
        send_w(2, 1, 2, 0).wait_send()
        send_w(0, 0, 3, 1).wait_send()
        send_w(1, 0, 3, 0).wait_send()
        spread_rounded(3, False)

    part_copy(partner).wait_send()
    for mask in order:
        for c in range(members):
            part_copy(flipped(mask) * members + c).wait_send()


def shards(integrals, densities, screen, factor, diag_inv):
    n_aux, n_pair = lax.axis_size("aux"), lax.axis_size("pair")
    height, width = integrals.shape
    breadth, block = factor.shape[1], diag_inv.shape[1]
    count = densities.shape[0]
    members, pieces = block // height, breadth // height
    share = width // n_aux
    vmem, dma = pltpu.VMEM, pltpu.SemaphoreType.DMA

    def rows(*lead):
        return vmem(lead + (count, height), F32)

    def whole(*lead, kind=F32):
        return vmem(lead + (count, block), kind)

    weights = 2 * block * block * 4 + 10 * block * block * 2
    fits = weights + integrals.size * 2 <= VMEM_ROOM
    if breadth == block and members == 2 and n_pair == SOLVE_BLOCKS and n_aux == 8 and fits:
        body = lead_kernel
        screen_space = pltpu.HBM
        scratch = [
            pltpu.SMEM(screen.shape, screen.dtype), vmem((height, width), BF16), vmem((count, width), BF16),
            vmem((block, block), F32), vmem((block, block), F32),
            *[vmem((block, block), BF16) for _ in range(10)],
            rows(), rows(n_pair, members), whole(kind=P_KIND), whole(n_pair, members, kind=P_KIND),
            whole(), whole(n_pair), whole(kind=S_KIND), whole(kind=S_KIND), whole(2), whole(),
            whole(2), whole(), whole(kind=V_KIND), whole(kind=V_KIND), whole(), whole(SOLVE_BLOCKS, n_pair),
            whole(), whole(), whole(), vmem((members, count, height), BF16),
            whole(kind=L_KIND), whole(kind=L_KIND),
            vmem((n_aux, count, share), BF16), vmem((n_aux, count, share), BF16),
            dma((width // LEAD_STREAM,)), dma((4,)),
            dma, dma((members,)), dma, dma((members,)),
            dma, dma((n_pair, members)), dma((2,)), dma((n_pair, members)), dma, dma((n_pair,)),
            dma, dma, dma((2,)), dma, dma((3,)), dma, dma, dma, dma, dma((SOLVE_BLOCKS, n_pair)),
            dma((members, n_pair)), dma, dma((members, n_pair)), dma,
            dma((n_aux,)), dma((n_aux,)),
        ]
    else:
        body = spread_kernel
        screen_space = pltpu.SMEM
        scratch = [
            vmem((height, width), BF16), vmem((count, width), BF16),
            vmem((height, breadth), F32), vmem((height, block), F32),
            vmem((height, breadth), BF16), vmem((height, breadth), BF16),
            vmem((height, block), BF16), vmem((height, block), BF16),
            rows(), rows(n_pair), rows(), rows(n_pair),
            rows(members), rows(members, pieces), rows(pieces), rows(members, members),
            rows(members), rows(), rows(pieces), rows(n_aux, members),
            vmem((n_aux, count, share), BF16), vmem((n_aux, count, share), BF16),
            dma((width // STREAM,)), dma((3,)),
            dma, dma((n_pair,)), dma, dma((n_pair,)),
            dma((members, n_aux)), dma((members, pieces)),
            dma((members, members)), dma((members, members)),
            dma((n_pair,)), dma, dma((pieces, members)), dma((n_aux, members)),
            dma((n_aux,)), dma((n_aux,)),
        ]
    return pl.pallas_call(
        functools.partial(body, n_aux, n_pair),
        out_shape=jax.ShapeDtypeStruct((count, share), F32),
        in_specs=[
            pl.BlockSpec(memory_space=pltpu.HBM),
            pl.BlockSpec(memory_space=pltpu.HBM),
            pl.BlockSpec(memory_space=screen_space),
            pl.BlockSpec(memory_space=pltpu.HBM),
            pl.BlockSpec(memory_space=pltpu.HBM),
        ],
        out_specs=pl.BlockSpec(memory_space=pltpu.VMEM),
        scratch_shapes=scratch,
        compiler_params=pltpu.CompilerParams(
            collective_id=0, has_side_effects=True, vmem_limit_bytes=VMEM_LIMIT if body is lead_kernel else 60 * 2**20
        ),
    )(integrals, densities, screen, factor, diag_inv)


def solution(mesh):
    in_specs = (
        P("aux", "pair"),
        P(None, "pair"),
        P("aux", "pair"),
        P("aux", "pair"),
        P("aux", None),
    )
    out_specs = P(None, ("pair", "aux"))
    return jax.shard_map(shards, mesh=mesh, in_specs=in_specs, out_specs=out_specs, check_vma=False)
```

```python
import functools

import jax
import jax.numpy as jnp
from jax import lax
from jax.experimental import pallas as pl
from jax.experimental.pallas import tpu as pltpu
from jax.sharding import PartitionSpec as P

TILE = 128
SOLVE_BLOCKS = 4
STREAM = 1024
LEAD_STREAM = 2048
VMEM_ROOM = 48 * 2**20
MESH = pl.DeviceIdType.MESH
NN = (((1,), (0,)), ((), ()))
NT = (((1,), (1,)), ((), ()))
F32 = jnp.float32
BF16 = jnp.bfloat16
P_KIND, S_KIND, V_KIND, L_KIND = BF16, BF16, BF16, BF16
VMEM_LIMIT = 44 * 2**20


def split(values):
    high = values.astype(BF16)
    return high, (values - high.astype(F32)).astype(BF16)


def dot_split(values, high, low, dims):
    top, rest = split(values)
    rows = values.shape[0]
    both = lax.dot_general(
        jnp.concatenate([top, rest], 0), high, dims, preferred_element_type=F32
    )
    minor = lax.dot_general(top, low, dims, preferred_element_type=F32)
    return both[:rows] + (both[rows:] + minor)


def spread_kernel(
    n_aux, n_pair,
    integrals, densities, screen, factor, diag_inv, out,
    masked, dens, fac, inv, fac_hi, fac_lo, inv_hi, inv_lo,
    fit_out, fit_in, u_out, u_in, s_out, s_in, s_sum, own_in, resid, coef, v_out, v_in,
    part_out, part_in,
    load_sem, small_sem,
    fit_send, fit_recv, u_send, u_recv, s_send, s_recv, own_send, own_recv,
    coef_send, coef_recv, v_send, v_recv, part_send, part_recv,
):
    height, width = masked.shape
    breadth = fac.shape[1]
    block = inv.shape[1]
    members = block // height
    group = block // breadth
    pieces = breadth // height
    share = width // n_aux
    chunks = width // STREAM

    row = lax.axis_index("aux")
    col = lax.axis_index("pair")
    mine = row // members
    member = lax.rem(row, members)
    column_block = col // group
    column_part = lax.rem(col, group)

    def home_of(k):
        return jnp.maximum(k - 1, 0) * group

    home = home_of(mine)
    is_home = col == home
    below = column_block < mine

    def remote(src, dst, send, recv, aux, pair):
        return pltpu.make_async_remote_copy(
            src_ref=src, dst_ref=dst, send_sem=send, recv_sem=recv,
            device_id={"aux": aux, "pair": pair}, device_id_type=MESH,
        )

    def load(c):
        at = pl.ds(pl.multiple_of(c * STREAM, STREAM), STREAM)
        return pltpu.make_async_copy(integrals.at[:, at], masked.at[:, at], load_sem.at[c])

    load_dens = pltpu.make_async_copy(densities, dens, small_sem.at[0])
    load_fac = pltpu.make_async_copy(factor, fac, small_sem.at[1])
    load_inv = pltpu.make_async_copy(diag_inv, inv, small_sem.at[2])
    load_dens.start()
    for c in range(chunks):
        load(c).start()
    load_inv.start()

    @pl.when(below)
    def _():
        load_fac.start()

    barrier = pltpu.get_barrier_semaphore()
    everyone = n_aux * n_pair
    me = row * n_pair + col

    def greet(i, carry):
        other = lax.rem(me + i, everyone)
        pl.semaphore_signal(
            barrier, inc=1,
            device_id={"aux": other // n_pair, "pair": lax.rem(other, n_pair)},
            device_id_type=MESH,
        )
        return carry

    lax.fori_loop(1, everyone, greet, 0)
    load_dens.wait()

    def fit_step(c, total):
        load(c).wait()
        base = pl.multiple_of(c * STREAM, STREAM)
        for r in range(height // TILE):
            for t in range(STREAM // TILE):
                flag = screen[r, c * (STREAM // TILE) + t].astype(F32)
                at = (pl.ds(r * TILE, TILE), pl.ds(pl.multiple_of(base + t * TILE, TILE), TILE))
                masked[at] = masked[at] * jnp.full((TILE, TILE), flag, F32).astype(BF16)
        span = pl.ds(base, STREAM)
        return total + lax.dot_general(
            dens[:, span], masked[:, span], NT, preferred_element_type=F32
        )

    fitted = lax.fori_loop(0, chunks, fit_step, jnp.zeros((dens.shape[0], height), F32))
    fit_out[...] = fitted
    pl.semaphore_wait(barrier, everyone - 1)

    send_fit = remote(fit_out, fit_in.at[col], fit_send, fit_recv.at[col], row, home)

    @pl.when(jnp.logical_not(is_home))
    def _():
        send_fit.start()

    load_inv.wait()
    high, low = split(inv[...])
    inv_hi[...] = high
    inv_lo[...] = low

    @pl.when(below)
    def _():
        load_fac.wait()
        high, low = split(fac[...])
        fac_hi[...] = high
        fac_lo[...] = low

    @pl.when(below)
    def _():
        for x in range(pieces):
            whole_x = column_part * pieces + x
            for c in range(members):
                @pl.when(whole_x >= c)
                def _():
                    remote(s_out.at[0], s_in.at[c, x], s_send.at[0, 0], s_recv.at[c, x], row, col).wait_recv()
                    if c == 0:
                        s_sum[x] = s_in[c, x]
                    else:
                        s_sum[x] += s_in[c, x]
        known = jnp.concatenate([s_sum[x] for x in range(pieces)], 1)
        u_out[...] = dot_split(known, fac_hi[...], fac_lo[...], NT)

        @pl.when(jnp.logical_not(is_home))
        def _():
            remote(u_out, u_in.at[col], u_send, u_recv.at[col], row, home).start()

    def send_solved(x, start):
        part, piece = x // pieces, x % pieces

        def later(d, carry):
            copy = remote(
                s_out.at[x], s_in.at[member, piece], s_send.at[x, d],
                s_recv.at[member, piece], d, mine * group + part,
            )
            copy.start() if start else copy.wait_send()
            return carry

        lax.fori_loop((mine + 1) * members, n_aux, later, 0)
        for i in range(1, members):
            other = lax.rem(member + i, members)

            @pl.when(other <= x)
            def _():
                copy = remote(
                    s_out.at[x], own_in.at[member, x], own_send.at[x, i],
                    own_recv.at[member, x], mine * members + other, home,
                )
                copy.start() if start else copy.wait_send()

    @pl.when(is_home)
    def _():
        fit_total = fit_out
        for p in range(n_pair):
            @pl.when(p != home)
            def _():
                remote(fit_out, fit_in.at[p], fit_send, fit_recv.at[p], row, col).wait_recv()
                fit_total[...] += fit_in[p]
        for p in range(n_pair):
            @pl.when(jnp.logical_and(p // group < mine, p != home))
            def _():
                remote(u_out, u_in.at[p], u_send, u_recv.at[p], row, col).wait_recv()
                fit_total[...] -= u_in[p]

        @pl.when(below)
        def _():
            fit_total[...] -= u_out[...]

        for x in range(members):
            @pl.when(x >= member)
            def _():
                at = pl.ds(x * height, height)
                s_out[x] = dot_split(fit_total[...], inv_hi[:, at], inv_lo[:, at], NN)
                send_solved(x, True)

        for x in range(members):
            @pl.when(x >= member)
            def _():
                resid[x] = s_out[x]
                for i in range(1, members):
                    other = lax.rem(member + i, members)

                    @pl.when(other <= x)
                    def _():
                        remote(s_out.at[0], own_in.at[other, x], own_send.at[0, 0], own_recv.at[other, x], row, col).wait_recv()
                        resid[x] += own_in[other, x]

        def subtract(i, carry):
            source = n_aux - 1 - i
            for x in range(members):
                @pl.when(x >= member)
                def _():
                    remote(v_out.at[0], v_in.at[source, x], v_send.at[0, 0], v_recv.at[source, x], row, col).wait_recv()
                    resid[x] -= v_in[source, x]
            return carry

        lax.fori_loop(0, n_aux - (mine + 1) * members, subtract, 0)
        for x in reversed(range(members)):
            @pl.when(x >= member)
            def _():
                at = pl.ds(x * height, height)
                term = dot_split(resid[x], inv_hi[:, at], inv_lo[:, at], NT)
                if x == members - 1:
                    coef[...] = term
                else:
                    coef[...] += term

        for i in range(1, n_pair):
            remote(coef, coef, coef_send.at[i], coef_recv, row, lax.rem(col + i, n_pair)).start()

    @pl.when(jnp.logical_not(is_home))
    def _():
        remote(coef, coef, coef_send.at[0], coef_recv, row, col).wait_recv()

    def send_v(x, start):
        whole_x = column_part * pieces + x
        for c in range(members):
            @pl.when(c <= whole_x)
            def _():
                copy = remote(
                    v_out.at[x], v_in.at[row, whole_x], v_send.at[x, c],
                    v_recv.at[row, whole_x], column_block * members + c, home_of(column_block),
                )
                copy.start() if start else copy.wait_send()

    @pl.when(below)
    def _():
        for x in range(pieces):
            at = pl.ds(x * height, height)
            v_out[x] = dot_split(coef[...], fac_hi[:, at], fac_lo[:, at], NN)
            send_v(x, True)

    rounded = coef[...].astype(BF16)

    def product(target):
        span = pl.ds(pl.multiple_of(target * share, TILE), share)
        return lax.dot_general(rounded, masked[:, span], NN, preferred_element_type=F32)

    def part_copy(i):
        target = lax.rem(row + i, n_aux)
        return target, remote(
            part_out.at[target], part_in.at[row], part_send.at[target], part_recv.at[row], target, col
        )

    def give(i, carry):
        target, copy = part_copy(i)
        part_out[target] = product(target).astype(BF16)
        copy.start()
        return carry

    lax.fori_loop(1, n_aux, give, 0)
    total = product(row)

    def take(i, total):
        source = lax.rem(row + n_aux - i, n_aux)
        remote(part_out.at[0], part_in.at[source], part_send.at[0], part_recv.at[source], row, col).wait_recv()
        return total + part_in[source].astype(F32)

    out[...] = lax.fori_loop(1, n_aux, take, total)

    @pl.when(jnp.logical_not(is_home))
    def _():
        send_fit.wait_send()

        @pl.when(below)
        def _():
            remote(u_out, u_in.at[col], u_send, u_recv.at[col], row, home).wait_send()

    @pl.when(is_home)
    def _():
        for x in range(members):
            @pl.when(x >= member)
            def _():
                send_solved(x, False)
        for i in range(1, n_pair):
            remote(coef, coef, coef_send.at[i], coef_recv, row, lax.rem(col + i, n_pair)).wait_send()

    @pl.when(below)
    def _():
        for x in range(pieces):
            send_v(x, False)

    def sent(i, carry):
        part_copy(i)[1].wait_send()
        return carry

    lax.fori_loop(1, n_aux, sent, 0)


def dot_two(values, high, low, dims):
    return lax.dot_general(values, high, dims, preferred_element_type=F32) + lax.dot_general(
        values, low, dims, preferred_element_type=F32
    )


def apply(values, high, low, dims):
    return (dot_two if values.dtype == BF16 else dot_split)(values, high, low, dims)


def lead_kernel(
    n_aux, n_pair,
    integrals, densities, screen, factor, diag_inv, out,
    flags, masked, dens, fac, inv, fac_hi, fac_lo, inv_hi, inv_lo, inv_t_hi, inv_t_lo,
    step_hi, step_lo, step_t_hi, step_t_lo,
    fit_out, fit_in, p_out, p_in, u_out, u_in, s_out, s_in, t_out, t_in, x_out, w_out, w_in, v_out, v_in, y_out, y_in,
    resid, solved, start, rounded, last_out, last_in, part_out, part_in,
    load_sem, small_sem, fac_send, fac_recv, inv_send, inv_recv,
    fit_send, fit_recv, p_send, p_recv, u_send, u_recv, s_send, s_recv, t_send, t_recv, x_send, w_send, w_recv,
    v_send, v_recv, y_send, y_recv, round_send, round_recv, last_send, last_recv, part_send, part_recv,
):
    height, width = masked.shape
    block = inv.shape[1]
    count = dens.shape[0]
    members = block // height
    share = width // n_aux
    chunks = width // STREAM
    wide = LEAD_STREAM // STREAM
    tail = chunks - wide
    strips = height // TILE

    row = lax.axis_index("aux")
    col = lax.axis_index("pair")
    mine = row // members
    member = lax.rem(row, members)
    lead = members - 1
    lead_row = mine * members + lead
    is_lead = member == lead
    first = mine == 0
    later = mine > 0
    home = jnp.maximum(mine - 1, 0)
    at_home = jnp.logical_and(later, col == home)
    below = col < mine

    def chip(k, z):
        return jnp.logical_and(mine == k, col == z)

    def role(k, z):
        return jnp.logical_and(is_lead, chip(k, z))

    lead_home = jnp.logical_and(is_lead, at_home)
    lead_below = jnp.logical_and(is_lead, below)

    def remote(src, dst, send, recv, aux, pair):
        return pltpu.make_async_remote_copy(
            src_ref=src, dst_ref=dst, send_sem=send, recv_sem=recv,
            device_id={"aux": aux, "pair": pair}, device_id_type=MESH,
        )

    def to_lead(src, dst, send, recv, k, z):
        return remote(src, dst, send, recv, k * members + lead, z)

    def load(c):
        at = pl.ds(pl.multiple_of(c * STREAM, STREAM), STREAM)
        return pltpu.make_async_copy(integrals.at[:, at], masked.at[:, at], load_sem.at[c])

    own = pl.ds(lead * height, height)
    load_dens = pltpu.make_async_copy(densities, dens, small_sem.at[0])
    load_fac = pltpu.make_async_copy(factor, fac.at[own], small_sem.at[1])
    load_inv = pltpu.make_async_copy(diag_inv, inv.at[own], small_sem.at[2])
    load_flags = pltpu.make_async_copy(screen, flags, small_sem.at[3])

    def move_fac(c):
        return remote(factor, fac.at[pl.ds(c * height, height)], fac_send, fac_recv.at[c], lead_row, col)

    def move_inv(c):
        right = pl.ds(c * height, block - c * height)
        return remote(
            diag_inv.at[:, right], inv.at[pl.ds(c * height, height), right],
            inv_send, inv_recv.at[c], lead_row, col,
        )

    def load_start(c):
        right = pl.ds(c * height, block - c * height)
        return pltpu.make_async_copy(diag_inv.at[:, right], inv.at[own, right], small_sem.at[2])

    load_flags.start()
    load_dens.start()
    for c in range(chunks):
        load(c).start()
    for c in range(members):
        @pl.when(jnp.logical_and(first, member == c))
        def _():
            load_start(c).start()


    @pl.when(lead_below)
    def _():
        load_fac.start()
        load_inv.start()

    barrier = pltpu.get_barrier_semaphore()

    def greet(k, c, z):
        pl.semaphore_signal(
            barrier, inc=1, device_id={"aux": k * members + c, "pair": z}, device_id_type=MESH
        )

    c_one, c_two, c_three = role(1, 0), role(2, 1), role(3, 2)
    lead_aside = jnp.logical_and(lead_below, jnp.logical_not(at_home))

    @pl.when(jnp.logical_or(c_one, role(2, 0)))
    def _():
        for c in range(members):
            for z in range(n_pair):
                greet(0, c, z)

    @pl.when(lead_home)
    def _():
        for c in range(members):
            for i in range(n_pair):
                if c != lead or i:
                    greet(mine, c, lax.rem(col + i, n_pair))

    @pl.when(lead_aside)
    def _():
        for c in range(lead):
            greet(mine, c, col)

    @pl.when(jnp.logical_or(c_two, jnp.logical_and(lead_aside, mine == 3)))
    def _():
        greet(1, lead, 0)

    @pl.when(c_three)
    def _():
        greet(2, lead, 1)

    gives = jnp.logical_and(jnp.logical_not(is_lead), below)
    greeted = (
        jnp.where(first, 2, 0)
        + jnp.where(jnp.logical_and(later, jnp.logical_not(lead_home)), 1, 0)
        + jnp.where(jnp.logical_and(gives, jnp.logical_not(at_home)), 1, 0)
        + jnp.where(c_one, 3, 0)
        + jnp.where(c_two, 1, 0)
    )

    @pl.when(gives)
    def _():
        pl.semaphore_wait(barrier, greeted)

    for c in range(lead):
        @pl.when(jnp.logical_and(gives, member == c))
        def _():
            move_fac(c).start()
            move_inv(c).start()

    load_flags.wait()
    load_dens.wait()

    def flag_of(r, t):
        return flags[r, t].astype(F32)

    def fit_step(c, steps, sums):
        size = steps * STREAM
        base = pl.multiple_of(c * STREAM, STREAM)
        kept = []
        for r in range(strips):
            tiles = []
            for t in range(size // TILE):
                at = pl.ds(pl.multiple_of(base + t * TILE, TILE), TILE)
                flag = flag_of(r, c * (STREAM // TILE) + t)
                tiles.append(dens[:, at] * jnp.full((count, TILE), flag, F32).astype(BF16))
            kept.append(jnp.concatenate(tiles, 1))
        for i in range(steps):
            load(c + i).wait()
        return tuple(
            sums[r] + lax.dot_general(
                kept[r], masked[pl.ds(r * TILE, TILE), pl.ds(base, size)], NT,
                preferred_element_type=F32,
            )
            for r in range(strips)
        )

    sums = lax.fori_loop(
        0, tail // wide, lambda i, sums: fit_step(i * wide, wide, sums),
        tuple(jnp.zeros((count, TILE), F32) for _ in range(strips)),
    )
    for c in range(members):
        @pl.when(jnp.logical_and(first, member == c))
        def _():
            right = pl.ds(c * height, block - c * height)
            load_start(c).wait()
            inv_hi[own, right], inv_lo[own, right] = split(inv[own, right])

    for c in range(tail, chunks):
        sums = fit_step(c, 1, sums)
    for r in range(strips):
        fit_out[:, pl.ds(r * TILE, TILE)] = sums[r]

    p_targets = ((1, 0), (2, 0))

    def send_p(c, i):
        right = pl.ds(c * height, block - c * height)
        return to_lead(
            p_out.at[:, right], p_in.at[col, c, :, right], p_send.at[i], p_recv.at[col, c], *p_targets[i]
        )

    for c in range(members):
        @pl.when(jnp.logical_and(first, member == c))
        def _():
            right = pl.ds(c * height, block - c * height)
            p_out[:, right] = dot_split(
                fit_out[...], inv_hi[own, right], inv_lo[own, right], NN
            ).astype(p_out.dtype)

    @pl.when(jnp.logical_not(jnp.logical_or(gives, c_three)))
    def _():
        pl.semaphore_wait(barrier, greeted)


    for c in range(members):
        @pl.when(jnp.logical_and(first, member == c))
        def _():
            for i in range(len(p_targets)):
                send_p(c, i).start()

    send_fit = remote(
        fit_out, fit_in.at[col, member], fit_send, fit_recv.at[col, member], lead_row, home
    )
    sends_fit = jnp.logical_and(later, jnp.logical_not(lead_home))

    @pl.when(sends_fit)
    def _():
        send_fit.start()

    def mask_step(c, carry):
        base = pl.multiple_of(c * STREAM, STREAM)
        for r in range(strips):
            for t in range(STREAM // TILE):
                flag = flag_of(r, c * (STREAM // TILE) + t)
                at = (pl.ds(r * TILE, TILE), pl.ds(pl.multiple_of(base + t * TILE, TILE), TILE))
                masked[at] = masked[at] * jnp.full((TILE, TILE), flag, F32).astype(BF16)
        return carry

    lax.fori_loop(0, chunks, mask_step, 0)

    for c in range(members):
        @pl.when(jnp.logical_and(first, member == c))
        def _():
            right = pl.ds(c * height, block - c * height)
            inv_t_hi[right, :height], inv_t_lo[right, :height] = split(inv[own, right].T)

    @pl.when(lead_below)
    def _():
        load_fac.wait()
        for c in range(lead):
            move_fac(c).wait_recv()
        fac_hi[...], fac_lo[...] = split(fac[...])
        load_inv.wait()
        for c in range(lead):
            move_inv(c).wait_recv()
        inv_hi[...], inv_lo[...] = split(inv[...])

    def prepare_back():
        inv_t_hi[...], inv_t_lo[...] = split(inv[...].T)
        whole = lax.dot_general(inv_t_hi[...], fac_hi[...], NN, preferred_element_type=F32)
        whole += lax.dot_general(inv_t_lo[...], fac_hi[...], NN, preferred_element_type=F32)
        whole += lax.dot_general(inv_t_hi[...], fac_lo[...], NN, preferred_element_type=F32)
        step_t_hi[...], step_t_lo[...] = split(whole)
        return whole

    def prepare_ahead():
        whole = prepare_back()
        step_hi[...], step_lo[...] = split(whole.T)

    def turn_fac():
        step_hi[...], step_lo[...] = split(fac[...].T)

    def gather_fit():
        resid[:, own] = fit_out[...]
        for c in range(lead):
            for p in range(n_pair):
                @pl.when(p == home)
                def _():
                    remote(fit_out, fit_in.at[p, c], fit_send, fit_recv.at[p, c], row, col).wait_recv()
                    resid[:, pl.ds(c * height, height)] = fit_in[p, c]
        for p in range(n_pair):
            for c in range(members):
                @pl.when(p != home)
                def _():
                    remote(fit_out, fit_in.at[p, c], fit_send, fit_recv.at[p, c], row, col).wait_recv()
                    resid[:, pl.ds(c * height, height)] += fit_in[p, c]

    def gather_start():
        for p in range(n_pair):
            for c in range(members):
                right = pl.ds(c * height, block - c * height)
                remote(
                    p_out.at[:, right], p_in.at[p, c, :, right], p_send.at[0], p_recv.at[p, c], row, col
                ).wait_recv()
        for c in range(members):
            at = pl.ds(c * height, height)
            sum_p = p_in[0, 0, :, at].astype(F32)
            for p in range(n_pair):
                for d in range(c + 1):
                    if p or d:
                        sum_p += p_in[p, d, :, at].astype(F32)
            start[:, at] = sum_p

    def send_s(k, z):
        return to_lead(s_out, s_in, s_send, s_recv, k, z)

    def send_x():
        return to_lead(x_out, s_in, x_send, s_recv, 2, 0)

    def send_t(slot, k, z):
        return to_lead(t_out.at[slot], t_in, t_send.at[slot], t_recv, k, z)

    def send_u(k):
        return to_lead(u_out, u_in.at[col], u_send, u_recv.at[col], k, k - 1)

    def send_v(k, z):
        return to_lead(v_out, v_in, v_send, v_recv, k, z)

    def send_y():
        return to_lead(y_out, y_in.at[mine, col], y_send, y_recv.at[mine, col], 1, 0)

    def send_w(i, k, z):
        return to_lead(w_out, w_in, w_send.at[i], w_recv, k, z)

    def wait_s():
        send_s(0, 0).wait_recv()

    def take_u(p):
        remote(u_out, u_in.at[p], u_send, u_recv.at[p], row, col).wait_recv()
        resid[...] -= u_in[p].astype(F32)

    def take_v():
        remote(v_out, v_in, v_send, v_recv, row, col).wait_recv()
        return v_in[...].astype(F32)

    def take_y(k, z):
        remote(y_out, y_in.at[k, z], y_send, y_recv.at[k, z], row, col).wait_recv()
        return y_in[k, z]

    def wait_w():
        send_w(0, 0, 0).wait_recv()

    def round_copy(k, c, i, z):
        return remote(
            rounded.at[c], rounded.at[c], round_send.at[c, i], round_recv, k * members + c, lax.rem(z + i, n_pair)
        )

    def spread_rounded(k, go):
        for i in reversed(range(n_pair)):
            for c in range(members):
                if c != lead or i:
                    copy = round_copy(k, c, i, k - 1)
                    copy.start() if go else copy.wait_send()

    def finish(k, values):
        coef = dot_split(values, inv_t_hi[...], inv_t_lo[...], NN)
        for c in range(members):
            rounded[c] = coef[:, c * height:(c + 1) * height].astype(BF16)
        spread_rounded(k, True)

    def last_copy(c, z):
        right = pl.ds(c * height, block - c * height)
        return remote(
            last_out.at[:, right], last_in.at[:, right], last_send.at[c, z], last_recv, c, z
        )

    @pl.when(role(1, 0))
    def _():
        turn_fac()
        gather_fit()
        gather_start()
        t_out[0] = start[...]
        send_t(0, 3, 0).start()
        resid[...] -= dot_split(start[...], step_hi[...], step_lo[...], NN)
        solved[...] = dot_split(resid[...], inv_hi[...], inv_lo[...], NN)
        s_out[...] = solved[...].astype(s_out.dtype)
        t_out[1] = solved[...]
        send_s(2, 1).start()
        send_t(1, 3, 1).start()
        prepare_back()
        solved[...] -= take_y(3, 1)
        start[...] -= take_y(3, 0)
        solved[...] -= take_v()
        back = dot_split(solved[...], step_t_hi[...], step_t_lo[...], NN)
        last_out[...] = (start[...] - take_y(2, 0) - back).astype(last_out.dtype)
        for z in reversed(range(n_pair)):
            for c in range(members):
                last_copy(c, z).start()
        finish(1, solved[...])

    @pl.when(role(2, 0))
    def _():
        turn_fac()
        gather_start()
        u_out[...] = dot_split(start[...], step_hi[...], step_lo[...], NN)
        send_u(2).start()
        prepare_back()
        wait_s()
        y_out[...] = apply(s_in[...], step_t_hi[...], step_t_lo[...], NN)
        send_y().start()

    @pl.when(jnp.logical_or(role(3, 0), role(3, 1)))
    def _():
        prepare_ahead()
        send_t(0, 0, 0).wait_recv()
        u_out[...] = dot_split(t_in[...], step_hi[...], step_lo[...], NN)
        send_u(3).start()
        wait_w()
        y_out[...] = dot_split(w_in[...], step_t_hi[...], step_t_lo[...], NN)
        send_y().start()

    @pl.when(role(2, 1))
    def _():
        prepare_ahead()
        gather_fit()
        take_u(0)
        resid[...] = dot_split(resid[...], inv_hi[...], inv_lo[...], NN)
        wait_s()
        solved[...] = resid[...] - apply(s_in[...], step_hi[...], step_lo[...], NN)
        s_out[...] = solved[...].astype(s_out.dtype)
        send_s(3, 2).start()
        solved[...] -= take_v()
        v_out[...] = dot_split(solved[...], step_t_hi[...], step_t_lo[...], NN).astype(v_out.dtype)
        send_v(1, 0).start()
        finish(2, solved[...])

    @pl.when(role(3, 2))
    def _():
        prepare_ahead()
        gather_fit()
        resid[...] = dot_split(resid[...], inv_hi[...], inv_lo[...], NN)
        take_u(0)
        take_u(1)
        wait_s()
        solved[...] = resid[...] - apply(s_in[...], step_hi[...], step_lo[...], NN)
        w_out[...] = solved[...]
        send_w(0, 3, 1).start()
        send_w(1, 3, 0).start()
        back = dot_split(solved[...], step_t_hi[...], step_t_lo[...], NN)
        v_out[...] = back.astype(v_out.dtype)
        send_v(2, 1).start()
        x_out[...] = (s_in[...].astype(F32) - back).astype(x_out.dtype)
        send_x().start()
        coef = dot_split(solved[...], inv_t_hi[...], inv_t_lo[...], NN)
        for c in range(members):
            rounded[c] = coef[:, c * height:(c + 1) * height].astype(BF16)
        spread_rounded(3, True)

    @pl.when(jnp.logical_and(later, jnp.logical_not(lead_home)))
    def _():
        remote(rounded.at[0], rounded.at[0], round_send.at[0, 0], round_recv, row, col).wait_recv()

    for c in range(members):
        @pl.when(jnp.logical_and(first, member == c))
        def _():
            right = pl.ds(c * height, block - c * height)
            remote(
                last_out.at[:, right], last_in.at[:, right], last_send.at[c, 0], last_recv, row, col
            ).wait_recv()
            rounded[c] = apply(
                last_in[:, right], inv_t_hi[right, :height], inv_t_lo[right, :height], NN
            ).astype(BF16)

    mine_rounded = rounded[member]

    span = members * share

    def product(group):
        at = pl.ds(pl.multiple_of(group * span, TILE), span)
        return lax.dot_general(mine_rounded, masked[:, at], NN, preferred_element_type=F32)

    def flipped(mask):
        group, unit = 0, 1
        while unit * members < n_aux:
            digit = lax.rem(mine // unit, 2)
            group = group + unit * (1 - digit if mask & unit else digit)
            unit *= 2
        return group

    order = sorted(range(1, n_aux // members), key=lambda m: -bin(m).count("1"))
    partner = mine * members + 1 - member

    def part_copy(target):
        return remote(
            part_out.at[target], part_in.at[row], part_send.at[target], part_recv.at[row], target, col
        )

    for mask in order:
        group = flipped(mask)
        values = product(group)
        for c in range(members):
            part_out[group * members + c] = values[:, c * share:(c + 1) * share].astype(BF16)
            part_copy(group * members + c).start()

    values = product(mine)
    halves = values[:, :share], values[:, share:]
    part_out[partner] = jnp.where(member == 0, halves[1], halves[0]).astype(BF16)
    part_copy(partner).start()
    total = jnp.where(member == 0, halves[0], halves[1])

    def take(source):
        remote(part_out.at[0], part_in.at[source], part_send.at[0], part_recv.at[source], row, col).wait_recv()
        return part_in[source].astype(F32)

    total += take(partner)
    for mask in reversed(order):
        for c in range(members):
            total += take(flipped(mask) * members + c)

    out[...] = total

    for c in range(lead):
        @pl.when(member == c)
        def _():
            @pl.when(below)
            def _():
                move_fac(c).wait_send()
                move_inv(c).wait_send()

    for c in range(members):
        @pl.when(jnp.logical_and(first, member == c))
        def _():
            for i in range(len(p_targets)):
                send_p(c, i).wait_send()

    @pl.when(sends_fit)
    def _():
        send_fit.wait_send()

    @pl.when(role(1, 0))
    def _():
        send_t(0, 3, 0).wait_send()
        send_s(2, 1).wait_send()
        send_t(1, 3, 1).wait_send()
        for z in range(n_pair):
            for c in range(members):
                last_copy(c, z).wait_send()
        spread_rounded(1, False)

    @pl.when(role(2, 0))
    def _():
        send_u(2).wait_send()
        send_y().wait_send()

    @pl.when(jnp.logical_or(role(3, 0), role(3, 1)))
    def _():
        send_u(3).wait_send()
        send_y().wait_send()

    @pl.when(role(2, 1))
    def _():
        send_s(3, 2).wait_send()
        send_v(1, 0).wait_send()
        spread_rounded(2, False)

    @pl.when(role(3, 2))
    def _():
        send_v(2, 1).wait_send()
        send_x().wait_send()
        send_w(0, 3, 1).wait_send()
        send_w(1, 3, 0).wait_send()
        spread_rounded(3, False)

    part_copy(partner).wait_send()
    for mask in order:
        for c in range(members):
            part_copy(flipped(mask) * members + c).wait_send()


def shards(integrals, densities, screen, factor, diag_inv):
    n_aux, n_pair = lax.axis_size("aux"), lax.axis_size("pair")
    height, width = integrals.shape
    breadth, block = factor.shape[1], diag_inv.shape[1]
    count = densities.shape[0]
    members, pieces = block // height, breadth // height
    share = width // n_aux
    vmem, dma = pltpu.VMEM, pltpu.SemaphoreType.DMA

    def rows(*lead):
        return vmem(lead + (count, height), F32)

    def whole(*lead, kind=F32):
        return vmem(lead + (count, block), kind)

    weights = 2 * block * block * 4 + 10 * block * block * 2
    fits = weights + integrals.size * 2 <= VMEM_ROOM
    if breadth == block and members == 2 and n_pair == SOLVE_BLOCKS and n_aux == 8 and fits:
        body = lead_kernel
        screen_space = pltpu.HBM
        scratch = [
            pltpu.SMEM(screen.shape, screen.dtype), vmem((height, width), BF16), vmem((count, width), BF16),
            vmem((block, block), F32), vmem((block, block), F32),
            *[vmem((block, block), BF16) for _ in range(10)],
            rows(), rows(n_pair, members), whole(kind=P_KIND), whole(n_pair, members, kind=P_KIND),
            whole(), whole(n_pair), whole(kind=S_KIND), whole(kind=S_KIND), whole(2), whole(),
            whole(kind=S_KIND), whole(), whole(), whole(kind=V_KIND), whole(kind=V_KIND),
            whole(), whole(SOLVE_BLOCKS, n_pair),
            whole(), whole(), whole(), vmem((members, count, height), BF16),
            whole(kind=L_KIND), whole(kind=L_KIND),
            vmem((n_aux, count, share), BF16), vmem((n_aux, count, share), BF16),
            dma((width // STREAM,)), dma((4,)),
            dma, dma((members,)), dma, dma((members,)),
            dma, dma((n_pair, members)), dma((2,)), dma((n_pair, members)), dma, dma((n_pair,)),
            dma, dma, dma((2,)), dma, dma, dma((2,)), dma, dma, dma, dma, dma((SOLVE_BLOCKS, n_pair)),
            dma((members, n_pair)), dma, dma((members, n_pair)), dma,
            dma((n_aux,)), dma((n_aux,)),
        ]
    else:
        body = spread_kernel
        screen_space = pltpu.SMEM
        scratch = [
            vmem((height, width), BF16), vmem((count, width), BF16),
            vmem((height, breadth), F32), vmem((height, block), F32),
            vmem((height, breadth), BF16), vmem((height, breadth), BF16),
            vmem((height, block), BF16), vmem((height, block), BF16),
            rows(), rows(n_pair), rows(), rows(n_pair),
            rows(members), rows(members, pieces), rows(pieces), rows(members, members),
            rows(members), rows(), rows(pieces), rows(n_aux, members),
            vmem((n_aux, count, share), BF16), vmem((n_aux, count, share), BF16),
            dma((width // STREAM,)), dma((3,)),
            dma, dma((n_pair,)), dma, dma((n_pair,)),
            dma((members, n_aux)), dma((members, pieces)),
            dma((members, members)), dma((members, members)),
            dma((n_pair,)), dma, dma((pieces, members)), dma((n_aux, members)),
            dma((n_aux,)), dma((n_aux,)),
        ]
    operands = integrals, densities, screen, factor, diag_inv
    if body is lead_kernel:
        operands = tuple(pltpu.with_memory_space_constraint(x, pltpu.HBM) for x in operands)
    return pl.pallas_call(
        functools.partial(body, n_aux, n_pair),
        out_shape=jax.ShapeDtypeStruct((count, share), F32),
        in_specs=[
            pl.BlockSpec(memory_space=pltpu.HBM),
            pl.BlockSpec(memory_space=pltpu.HBM),
            pl.BlockSpec(memory_space=screen_space),
            pl.BlockSpec(memory_space=pltpu.HBM),
            pl.BlockSpec(memory_space=pltpu.HBM),
        ],
        out_specs=pl.BlockSpec(memory_space=pltpu.VMEM),
        scratch_shapes=scratch,
        compiler_params=pltpu.CompilerParams(
            collective_id=0, has_side_effects=True, vmem_limit_bytes=VMEM_LIMIT if body is lead_kernel else 60 * 2**20
        ),
    )(*operands)


def solution(mesh):
    in_specs = (
        P("aux", "pair"),
        P(None, "pair"),
        P("aux", "pair"),
        P("aux", "pair"),
        P("aux", None),
    )
    out_specs = P(None, ("pair", "aux"))
    return jax.shard_map(shards, mesh=mesh, in_specs=in_specs, out_specs=out_specs, check_vma=False)
```

```python
import functools

import jax
import jax.numpy as jnp
from jax import lax
from jax.experimental import pallas as pl
from jax.experimental.pallas import tpu as pltpu
from jax.sharding import PartitionSpec as P

TILE = 128
SOLVE_BLOCKS = 4
STREAM = 1024
LEAD_STREAM = 2048
VMEM_ROOM = 48 * 2**20
MESH = pl.DeviceIdType.MESH
NN = (((1,), (0,)), ((), ()))
NT = (((1,), (1,)), ((), ()))
F32 = jnp.float32
BF16 = jnp.bfloat16
P_KIND, S_KIND, V_KIND, L_KIND = BF16, BF16, BF16, BF16
VMEM_LIMIT = 44 * 2**20


def split(values):
    high = values.astype(BF16)
    return high, (values - high.astype(F32)).astype(BF16)


def dot_split(values, high, low, dims):
    top, rest = split(values)
    rows = values.shape[0]
    both = lax.dot_general(
        jnp.concatenate([top, rest], 0), high, dims, preferred_element_type=F32
    )
    minor = lax.dot_general(top, low, dims, preferred_element_type=F32)
    return both[:rows] + (both[rows:] + minor)


def spread_kernel(
    n_aux, n_pair,
    integrals, densities, screen, factor, diag_inv, out,
    masked, dens, fac, inv, fac_hi, fac_lo, inv_hi, inv_lo,
    fit_out, fit_in, u_out, u_in, s_out, s_in, s_sum, own_in, resid, coef, v_out, v_in,
    part_out, part_in,
    load_sem, small_sem,
    fit_send, fit_recv, u_send, u_recv, s_send, s_recv, own_send, own_recv,
    coef_send, coef_recv, v_send, v_recv, part_send, part_recv,
):
    height, width = masked.shape
    breadth = fac.shape[1]
    block = inv.shape[1]
    members = block // height
    group = block // breadth
    pieces = breadth // height
    share = width // n_aux
    chunks = width // STREAM

    row = lax.axis_index("aux")
    col = lax.axis_index("pair")
    mine = row // members
    member = lax.rem(row, members)
    column_block = col // group
    column_part = lax.rem(col, group)

    def home_of(k):
        return jnp.maximum(k - 1, 0) * group

    home = home_of(mine)
    is_home = col == home
    below = column_block < mine

    def remote(src, dst, send, recv, aux, pair):
        return pltpu.make_async_remote_copy(
            src_ref=src, dst_ref=dst, send_sem=send, recv_sem=recv,
            device_id={"aux": aux, "pair": pair}, device_id_type=MESH,
        )

    def load(c):
        at = pl.ds(pl.multiple_of(c * STREAM, STREAM), STREAM)
        return pltpu.make_async_copy(integrals.at[:, at], masked.at[:, at], load_sem.at[c])

    load_dens = pltpu.make_async_copy(densities, dens, small_sem.at[0])
    load_fac = pltpu.make_async_copy(factor, fac, small_sem.at[1])
    load_inv = pltpu.make_async_copy(diag_inv, inv, small_sem.at[2])
    load_dens.start()
    for c in range(chunks):
        load(c).start()
    load_inv.start()

    @pl.when(below)
    def _():
        load_fac.start()

    barrier = pltpu.get_barrier_semaphore()
    everyone = n_aux * n_pair
    me = row * n_pair + col

    def greet(i, carry):
        other = lax.rem(me + i, everyone)
        pl.semaphore_signal(
            barrier, inc=1,
            device_id={"aux": other // n_pair, "pair": lax.rem(other, n_pair)},
            device_id_type=MESH,
        )
        return carry

    lax.fori_loop(1, everyone, greet, 0)
    load_dens.wait()

    def fit_step(c, total):
        load(c).wait()
        base = pl.multiple_of(c * STREAM, STREAM)
        for r in range(height // TILE):
            for t in range(STREAM // TILE):
                flag = screen[r, c * (STREAM // TILE) + t].astype(F32)
                at = (pl.ds(r * TILE, TILE), pl.ds(pl.multiple_of(base + t * TILE, TILE), TILE))
                masked[at] = masked[at] * jnp.full((TILE, TILE), flag, F32).astype(BF16)
        span = pl.ds(base, STREAM)
        return total + lax.dot_general(
            dens[:, span], masked[:, span], NT, preferred_element_type=F32
        )

    fitted = lax.fori_loop(0, chunks, fit_step, jnp.zeros((dens.shape[0], height), F32))
    fit_out[...] = fitted
    pl.semaphore_wait(barrier, everyone - 1)

    send_fit = remote(fit_out, fit_in.at[col], fit_send, fit_recv.at[col], row, home)

    @pl.when(jnp.logical_not(is_home))
    def _():
        send_fit.start()

    load_inv.wait()
    high, low = split(inv[...])
    inv_hi[...] = high
    inv_lo[...] = low

    @pl.when(below)
    def _():
        load_fac.wait()
        high, low = split(fac[...])
        fac_hi[...] = high
        fac_lo[...] = low

    @pl.when(below)
    def _():
        for x in range(pieces):
            whole_x = column_part * pieces + x
            for c in range(members):
                @pl.when(whole_x >= c)
                def _():
                    remote(s_out.at[0], s_in.at[c, x], s_send.at[0, 0], s_recv.at[c, x], row, col).wait_recv()
                    if c == 0:
                        s_sum[x] = s_in[c, x]
                    else:
                        s_sum[x] += s_in[c, x]
        known = jnp.concatenate([s_sum[x] for x in range(pieces)], 1)
        u_out[...] = dot_split(known, fac_hi[...], fac_lo[...], NT)

        @pl.when(jnp.logical_not(is_home))
        def _():
            remote(u_out, u_in.at[col], u_send, u_recv.at[col], row, home).start()

    def send_solved(x, start):
        part, piece = x // pieces, x % pieces

        def later(d, carry):
            copy = remote(
                s_out.at[x], s_in.at[member, piece], s_send.at[x, d],
                s_recv.at[member, piece], d, mine * group + part,
            )
            copy.start() if start else copy.wait_send()
            return carry

        lax.fori_loop((mine + 1) * members, n_aux, later, 0)
        for i in range(1, members):
            other = lax.rem(member + i, members)

            @pl.when(other <= x)
            def _():
                copy = remote(
                    s_out.at[x], own_in.at[member, x], own_send.at[x, i],
                    own_recv.at[member, x], mine * members + other, home,
                )
                copy.start() if start else copy.wait_send()

    @pl.when(is_home)
    def _():
        fit_total = fit_out
        for p in range(n_pair):
            @pl.when(p != home)
            def _():
                remote(fit_out, fit_in.at[p], fit_send, fit_recv.at[p], row, col).wait_recv()
                fit_total[...] += fit_in[p]
        for p in range(n_pair):
            @pl.when(jnp.logical_and(p // group < mine, p != home))
            def _():
                remote(u_out, u_in.at[p], u_send, u_recv.at[p], row, col).wait_recv()
                fit_total[...] -= u_in[p]

        @pl.when(below)
        def _():
            fit_total[...] -= u_out[...]

        for x in range(members):
            @pl.when(x >= member)
            def _():
                at = pl.ds(x * height, height)
                s_out[x] = dot_split(fit_total[...], inv_hi[:, at], inv_lo[:, at], NN)
                send_solved(x, True)

        for x in range(members):
            @pl.when(x >= member)
            def _():
                resid[x] = s_out[x]
                for i in range(1, members):
                    other = lax.rem(member + i, members)

                    @pl.when(other <= x)
                    def _():
                        remote(s_out.at[0], own_in.at[other, x], own_send.at[0, 0], own_recv.at[other, x], row, col).wait_recv()
                        resid[x] += own_in[other, x]

        def subtract(i, carry):
            source = n_aux - 1 - i
            for x in range(members):
                @pl.when(x >= member)
                def _():
                    remote(v_out.at[0], v_in.at[source, x], v_send.at[0, 0], v_recv.at[source, x], row, col).wait_recv()
                    resid[x] -= v_in[source, x]
            return carry

        lax.fori_loop(0, n_aux - (mine + 1) * members, subtract, 0)
        for x in reversed(range(members)):
            @pl.when(x >= member)
            def _():
                at = pl.ds(x * height, height)
                term = dot_split(resid[x], inv_hi[:, at], inv_lo[:, at], NT)
                if x == members - 1:
                    coef[...] = term
                else:
                    coef[...] += term

        for i in range(1, n_pair):
            remote(coef, coef, coef_send.at[i], coef_recv, row, lax.rem(col + i, n_pair)).start()

    @pl.when(jnp.logical_not(is_home))
    def _():
        remote(coef, coef, coef_send.at[0], coef_recv, row, col).wait_recv()

    def send_v(x, start):
        whole_x = column_part * pieces + x
        for c in range(members):
            @pl.when(c <= whole_x)
            def _():
                copy = remote(
                    v_out.at[x], v_in.at[row, whole_x], v_send.at[x, c],
                    v_recv.at[row, whole_x], column_block * members + c, home_of(column_block),
                )
                copy.start() if start else copy.wait_send()

    @pl.when(below)
    def _():
        for x in range(pieces):
            at = pl.ds(x * height, height)
            v_out[x] = dot_split(coef[...], fac_hi[:, at], fac_lo[:, at], NN)
            send_v(x, True)

    rounded = coef[...].astype(BF16)

    def product(target):
        span = pl.ds(pl.multiple_of(target * share, TILE), share)
        return lax.dot_general(rounded, masked[:, span], NN, preferred_element_type=F32)

    def part_copy(i):
        target = lax.rem(row + i, n_aux)
        return target, remote(
            part_out.at[target], part_in.at[row], part_send.at[target], part_recv.at[row], target, col
        )

    def give(i, carry):
        target, copy = part_copy(i)
        part_out[target] = product(target).astype(BF16)
        copy.start()
        return carry

    lax.fori_loop(1, n_aux, give, 0)
    total = product(row)

    def take(i, total):
        source = lax.rem(row + n_aux - i, n_aux)
        remote(part_out.at[0], part_in.at[source], part_send.at[0], part_recv.at[source], row, col).wait_recv()
        return total + part_in[source].astype(F32)

    out[...] = lax.fori_loop(1, n_aux, take, total)

    @pl.when(jnp.logical_not(is_home))
    def _():
        send_fit.wait_send()

        @pl.when(below)
        def _():
            remote(u_out, u_in.at[col], u_send, u_recv.at[col], row, home).wait_send()

    @pl.when(is_home)
    def _():
        for x in range(members):
            @pl.when(x >= member)
            def _():
                send_solved(x, False)
        for i in range(1, n_pair):
            remote(coef, coef, coef_send.at[i], coef_recv, row, lax.rem(col + i, n_pair)).wait_send()

    @pl.when(below)
    def _():
        for x in range(pieces):
            send_v(x, False)

    def sent(i, carry):
        part_copy(i)[1].wait_send()
        return carry

    lax.fori_loop(1, n_aux, sent, 0)


def dot_two(values, high, low, dims):
    return lax.dot_general(values, high, dims, preferred_element_type=F32) + lax.dot_general(
        values, low, dims, preferred_element_type=F32
    )


def apply(values, high, low, dims):
    return (dot_two if values.dtype == BF16 else dot_split)(values, high, low, dims)


def lead_kernel(
    n_aux, n_pair,
    integrals, densities, screen, factor, diag_inv, out,
    flags, masked, dens, fac, inv, fac_hi, fac_lo, inv_hi, inv_lo, inv_t_hi, inv_t_lo,
    step_hi, step_lo, step_t_hi, step_t_lo,
    fit_out, fit_in, p_out, p_in, u_out, u_in, s_out, s_in, t_out, t_in, x_out, w_out, w_in, v_out, v_in, y_out, y_in,
    resid, solved, start, rounded, last_out, last_in, pair_out, pair_in, part_out, part_in,
    load_sem, small_sem, fac_send, fac_recv, inv_send, inv_recv,
    fit_send, fit_recv, p_send, p_recv, u_send, u_recv, s_send, s_recv, t_send, t_recv, x_send, w_send, w_recv,
    v_send, v_recv, y_send, y_recv, round_send, round_recv, last_send, last_recv, pair_send, pair_recv, part_send, part_recv,
):
    height, width = masked.shape
    block = inv.shape[1]
    count = dens.shape[0]
    members = block // height
    share = width // n_aux
    chunks = width // STREAM
    wide = LEAD_STREAM // STREAM
    tail = chunks - wide
    strips = height // TILE

    row = lax.axis_index("aux")
    col = lax.axis_index("pair")
    mine = row // members
    member = lax.rem(row, members)
    lead = members - 1
    lead_row = mine * members + lead
    is_lead = member == lead
    first = mine == 0
    later = mine > 0
    home = jnp.maximum(mine - 1, 0)
    at_home = jnp.logical_and(later, col == home)
    below = col < mine

    def chip(k, z):
        return jnp.logical_and(mine == k, col == z)

    def role(k, z):
        return jnp.logical_and(is_lead, chip(k, z))

    lead_home = jnp.logical_and(is_lead, at_home)
    lead_below = jnp.logical_and(is_lead, below)

    def remote(src, dst, send, recv, aux, pair):
        return pltpu.make_async_remote_copy(
            src_ref=src, dst_ref=dst, send_sem=send, recv_sem=recv,
            device_id={"aux": aux, "pair": pair}, device_id_type=MESH,
        )

    def to_lead(src, dst, send, recv, k, z):
        return remote(src, dst, send, recv, k * members + lead, z)

    def load(c):
        at = pl.ds(pl.multiple_of(c * STREAM, STREAM), STREAM)
        return pltpu.make_async_copy(integrals.at[:, at], masked.at[:, at], load_sem.at[c])

    own = pl.ds(lead * height, height)
    load_dens = pltpu.make_async_copy(densities, dens, small_sem.at[0])
    load_fac = pltpu.make_async_copy(factor, fac.at[own], small_sem.at[1])
    load_inv = pltpu.make_async_copy(diag_inv, inv.at[own], small_sem.at[2])
    load_flags = pltpu.make_async_copy(screen, flags, small_sem.at[3])

    def move_fac(c):
        return remote(factor, fac.at[pl.ds(c * height, height)], fac_send, fac_recv.at[c], lead_row, col)

    def move_inv(c):
        right = pl.ds(c * height, block - c * height)
        return remote(
            diag_inv.at[:, right], inv.at[pl.ds(c * height, height), right],
            inv_send, inv_recv.at[c], lead_row, col,
        )

    def load_start(c):
        right = pl.ds(c * height, block - c * height)
        return pltpu.make_async_copy(diag_inv.at[:, right], inv.at[own, right], small_sem.at[2])

    load_flags.start()
    load_dens.start()
    for c in range(chunks):
        load(c).start()
    for c in range(members):
        @pl.when(jnp.logical_and(first, member == c))
        def _():
            load_start(c).start()


    @pl.when(lead_below)
    def _():
        load_fac.start()
        load_inv.start()

    barrier = pltpu.get_barrier_semaphore()

    def greet(k, c, z):
        pl.semaphore_signal(
            barrier, inc=1, device_id={"aux": k * members + c, "pair": z}, device_id_type=MESH
        )

    c_one, c_two, c_three = role(1, 0), role(2, 1), role(3, 2)
    lead_aside = jnp.logical_and(lead_below, jnp.logical_not(at_home))

    @pl.when(jnp.logical_or(c_one, role(2, 0)))
    def _():
        for c in range(members):
            for z in range(n_pair):
                greet(0, c, z)

    @pl.when(lead_home)
    def _():
        for c in range(members):
            for i in range(n_pair):
                if c != lead or i:
                    greet(mine, c, lax.rem(col + i, n_pair))

    @pl.when(lead_aside)
    def _():
        for c in range(lead):
            greet(mine, c, col)

    @pl.when(jnp.logical_or(c_two, jnp.logical_and(lead_aside, mine == 3)))
    def _():
        greet(1, lead, 0)

    @pl.when(c_three)
    def _():
        greet(2, lead, 1)

    gives = jnp.logical_and(jnp.logical_not(is_lead), below)
    greeted = (
        jnp.where(first, 2, 0)
        + jnp.where(jnp.logical_and(later, jnp.logical_not(lead_home)), 1, 0)
        + jnp.where(jnp.logical_and(gives, jnp.logical_not(at_home)), 1, 0)
        + jnp.where(c_one, 3, 0)
        + jnp.where(c_two, 1, 0)
    )

    @pl.when(gives)
    def _():
        pl.semaphore_wait(barrier, greeted)

    for c in range(lead):
        @pl.when(jnp.logical_and(gives, member == c))
        def _():
            move_fac(c).start()
            move_inv(c).start()

    load_flags.wait()
    load_dens.wait()

    def flag_of(r, t):
        return flags[r, t].astype(F32)

    def fit_step(c, steps, sums):
        size = steps * STREAM
        base = pl.multiple_of(c * STREAM, STREAM)
        kept = []
        for r in range(strips):
            tiles = []
            for t in range(size // TILE):
                at = pl.ds(pl.multiple_of(base + t * TILE, TILE), TILE)
                flag = flag_of(r, c * (STREAM // TILE) + t)
                tiles.append(dens[:, at] * jnp.full((count, TILE), flag, F32).astype(BF16))
            kept.append(jnp.concatenate(tiles, 1))
        for i in range(steps):
            load(c + i).wait()
        return tuple(
            sums[r] + lax.dot_general(
                kept[r], masked[pl.ds(r * TILE, TILE), pl.ds(base, size)], NT,
                preferred_element_type=F32,
            )
            for r in range(strips)
        )

    sums = lax.fori_loop(
        0, tail // wide, lambda i, sums: fit_step(i * wide, wide, sums),
        tuple(jnp.zeros((count, TILE), F32) for _ in range(strips)),
    )
    for c in range(members):
        @pl.when(jnp.logical_and(first, member == c))
        def _():
            right = pl.ds(c * height, block - c * height)
            load_start(c).wait()
            inv_hi[own, right], inv_lo[own, right] = split(inv[own, right])

    for c in range(tail, chunks):
        sums = fit_step(c, 1, sums)
    for r in range(strips):
        fit_out[:, pl.ds(r * TILE, TILE)] = sums[r]

    p_targets = ((1, 0), (2, 0))

    def send_p(c, i):
        right = pl.ds(c * height, block - c * height)
        return to_lead(
            p_out.at[:, right], p_in.at[col, c, :, right], p_send.at[i], p_recv.at[col, c], *p_targets[i]
        )

    for c in range(members):
        @pl.when(jnp.logical_and(first, member == c))
        def _():
            right = pl.ds(c * height, block - c * height)
            p_out[:, right] = dot_split(
                fit_out[...], inv_hi[own, right], inv_lo[own, right], NN
            ).astype(p_out.dtype)

    @pl.when(jnp.logical_not(jnp.logical_or(gives, c_three)))
    def _():
        pl.semaphore_wait(barrier, greeted)


    for c in range(members):
        @pl.when(jnp.logical_and(first, member == c))
        def _():
            for i in range(len(p_targets)):
                send_p(c, i).start()

    send_fit = remote(
        fit_out, fit_in.at[col, member], fit_send, fit_recv.at[col, member], lead_row, home
    )
    sends_fit = jnp.logical_and(later, jnp.logical_not(lead_home))

    @pl.when(sends_fit)
    def _():
        send_fit.start()

    def mask_step(c, carry):
        base = pl.multiple_of(c * STREAM, STREAM)
        for r in range(strips):
            for t in range(STREAM // TILE):
                flag = flag_of(r, c * (STREAM // TILE) + t)
                at = (pl.ds(r * TILE, TILE), pl.ds(pl.multiple_of(base + t * TILE, TILE), TILE))
                masked[at] = masked[at] * jnp.full((TILE, TILE), flag, F32).astype(BF16)
        return carry

    lax.fori_loop(0, chunks, mask_step, 0)

    for c in range(members):
        @pl.when(jnp.logical_and(first, member == c))
        def _():
            right = pl.ds(c * height, block - c * height)
            inv_t_hi[right, :height], inv_t_lo[right, :height] = split(inv[own, right].T)

    @pl.when(lead_below)
    def _():
        load_fac.wait()
        for c in range(lead):
            move_fac(c).wait_recv()
        fac_hi[...], fac_lo[...] = split(fac[...])
        load_inv.wait()
        for c in range(lead):
            move_inv(c).wait_recv()
        inv_hi[...], inv_lo[...] = split(inv[...])

    def prepare_back():
        inv_t_hi[...], inv_t_lo[...] = split(inv[...].T)
        whole = lax.dot_general(inv_t_hi[...], fac_hi[...], NN, preferred_element_type=F32)
        whole += lax.dot_general(inv_t_lo[...], fac_hi[...], NN, preferred_element_type=F32)
        whole += lax.dot_general(inv_t_hi[...], fac_lo[...], NN, preferred_element_type=F32)
        step_t_hi[...], step_t_lo[...] = split(whole)
        return whole

    def prepare_ahead():
        whole = prepare_back()
        step_hi[...], step_lo[...] = split(whole.T)

    def turn_fac():
        step_hi[...], step_lo[...] = split(fac[...].T)

    def gather_fit():
        resid[:, own] = fit_out[...]
        for c in range(lead):
            for p in range(n_pair):
                @pl.when(p == home)
                def _():
                    remote(fit_out, fit_in.at[p, c], fit_send, fit_recv.at[p, c], row, col).wait_recv()
                    resid[:, pl.ds(c * height, height)] = fit_in[p, c]
        for p in range(n_pair):
            for c in range(members):
                @pl.when(p != home)
                def _():
                    remote(fit_out, fit_in.at[p, c], fit_send, fit_recv.at[p, c], row, col).wait_recv()
                    resid[:, pl.ds(c * height, height)] += fit_in[p, c]

    def gather_start():
        for p in range(n_pair):
            for c in range(members):
                right = pl.ds(c * height, block - c * height)
                remote(
                    p_out.at[:, right], p_in.at[p, c, :, right], p_send.at[0], p_recv.at[p, c], row, col
                ).wait_recv()
        for c in range(members):
            at = pl.ds(c * height, height)
            sum_p = p_in[0, 0, :, at].astype(F32)
            for p in range(n_pair):
                for d in range(c + 1):
                    if p or d:
                        sum_p += p_in[p, d, :, at].astype(F32)
            start[:, at] = sum_p

    def send_s(k, z):
        return to_lead(s_out, s_in, s_send, s_recv, k, z)

    def send_x():
        return to_lead(x_out, s_in, x_send, s_recv, 2, 0)

    def send_t(slot, k, z):
        return to_lead(t_out.at[slot], t_in, t_send.at[slot], t_recv, k, z)

    def send_u(k):
        return to_lead(u_out, u_in.at[col], u_send, u_recv.at[col], k, k - 1)

    def send_v(k, z):
        return to_lead(v_out, v_in, v_send, v_recv, k, z)

    def send_y():
        return to_lead(y_out, y_in.at[mine, col], y_send, y_recv.at[mine, col], 1, 0)

    def send_w(i, k, z):
        return to_lead(w_out, w_in, w_send.at[i], w_recv, k, z)

    def wait_s():
        send_s(0, 0).wait_recv()

    def take_u(p):
        remote(u_out, u_in.at[p], u_send, u_recv.at[p], row, col).wait_recv()
        resid[...] -= u_in[p].astype(F32)

    def take_v():
        remote(v_out, v_in, v_send, v_recv, row, col).wait_recv()
        return v_in[...].astype(F32)

    def take_y(k, z):
        remote(y_out, y_in.at[k, z], y_send, y_recv.at[k, z], row, col).wait_recv()
        return y_in[k, z]

    def wait_w():
        send_w(0, 0, 0).wait_recv()

    def round_copy(k, c, i, z):
        return remote(
            rounded.at[c], rounded.at[c], round_send.at[c, i], round_recv, k * members + c, lax.rem(z + i, n_pair)
        )

    def spread_rounded(k, go):
        for i in reversed(range(n_pair)):
            for c in range(members):
                if c != lead or i:
                    copy = round_copy(k, c, i, k - 1)
                    copy.start() if go else copy.wait_send()

    def finish(k, values):
        coef = dot_split(values, inv_t_hi[...], inv_t_lo[...], NN)
        for c in range(members):
            rounded[c] = coef[:, c * height:(c + 1) * height].astype(BF16)
        spread_rounded(k, True)

    def last_copy(c, z):
        right = pl.ds(c * height, block - c * height)
        return remote(
            last_out.at[:, right], last_in.at[:, right], last_send.at[c, z], last_recv, c, z
        )

    @pl.when(role(1, 0))
    def _():
        turn_fac()
        gather_fit()
        gather_start()
        t_out[0] = start[...]
        send_t(0, 3, 0).start()
        resid[...] -= dot_split(start[...], step_hi[...], step_lo[...], NN)
        solved[...] = dot_split(resid[...], inv_hi[...], inv_lo[...], NN)
        s_out[...] = solved[...].astype(s_out.dtype)
        t_out[1] = solved[...]
        send_s(2, 1).start()
        send_t(1, 3, 1).start()
        prepare_back()
        solved[...] -= take_y(3, 1)
        start[...] -= take_y(3, 0)
        solved[...] -= take_v()
        back = dot_split(solved[...], step_t_hi[...], step_t_lo[...], NN)
        last_out[...] = (start[...] - take_y(2, 0) - back).astype(last_out.dtype)
        for z in reversed(range(n_pair)):
            for c in range(members):
                last_copy(c, z).start()
        finish(1, solved[...])

    @pl.when(role(2, 0))
    def _():
        turn_fac()
        gather_start()
        u_out[...] = dot_split(start[...], step_hi[...], step_lo[...], NN)
        send_u(2).start()
        prepare_back()
        wait_s()
        y_out[...] = apply(s_in[...], step_t_hi[...], step_t_lo[...], NN)
        send_y().start()

    @pl.when(jnp.logical_or(role(3, 0), role(3, 1)))
    def _():
        prepare_ahead()
        send_t(0, 0, 0).wait_recv()
        u_out[...] = dot_split(t_in[...], step_hi[...], step_lo[...], NN)
        send_u(3).start()
        wait_w()
        y_out[...] = dot_split(w_in[...], step_t_hi[...], step_t_lo[...], NN)
        send_y().start()

    @pl.when(role(2, 1))
    def _():
        prepare_ahead()
        gather_fit()
        take_u(0)
        resid[...] = dot_split(resid[...], inv_hi[...], inv_lo[...], NN)
        wait_s()
        solved[...] = resid[...] - apply(s_in[...], step_hi[...], step_lo[...], NN)
        s_out[...] = solved[...].astype(s_out.dtype)
        send_s(3, 2).start()
        solved[...] -= take_v()
        v_out[...] = dot_split(solved[...], step_t_hi[...], step_t_lo[...], NN).astype(v_out.dtype)
        send_v(1, 0).start()
        finish(2, solved[...])

    @pl.when(role(3, 2))
    def _():
        prepare_ahead()
        gather_fit()
        resid[...] = dot_split(resid[...], inv_hi[...], inv_lo[...], NN)
        take_u(0)
        take_u(1)
        wait_s()
        solved[...] = resid[...] - apply(s_in[...], step_hi[...], step_lo[...], NN)
        w_out[...] = solved[...]
        send_w(0, 3, 1).start()
        send_w(1, 3, 0).start()
        back = dot_split(solved[...], step_t_hi[...], step_t_lo[...], NN)
        v_out[...] = back.astype(v_out.dtype)
        send_v(2, 1).start()
        x_out[...] = (s_in[...].astype(F32) - back).astype(x_out.dtype)
        send_x().start()
        coef = dot_split(solved[...], inv_t_hi[...], inv_t_lo[...], NN)
        for c in range(members):
            rounded[c] = coef[:, c * height:(c + 1) * height].astype(BF16)
        spread_rounded(3, True)

    @pl.when(jnp.logical_and(later, jnp.logical_not(lead_home)))
    def _():
        remote(rounded.at[0], rounded.at[0], round_send.at[0, 0], round_recv, row, col).wait_recv()

    for c in range(members):
        @pl.when(jnp.logical_and(first, member == c))
        def _():
            right = pl.ds(c * height, block - c * height)
            remote(
                last_out.at[:, right], last_in.at[:, right], last_send.at[c, 0], last_recv, row, col
            ).wait_recv()
            rounded[c] = apply(
                last_in[:, right], inv_t_hi[right, :height], inv_t_lo[right, :height], NN
            ).astype(BF16)

    mine_rounded = rounded[member]

    span = members * share

    def product(group):
        at = pl.ds(pl.multiple_of(group * span, TILE), span)
        return lax.dot_general(mine_rounded, masked[:, at], NN, preferred_element_type=F32)

    def flipped(mask):
        group, unit = 0, 1
        while unit * members < n_aux:
            digit = lax.rem(mine // unit, 2)
            group = group + unit * (1 - digit if mask & unit else digit)
            unit *= 2
        return group

    order = sorted(range(1, n_aux // members), key=lambda m: -bin(m).count("1"))
    partner = mine * members + 1 - member

    def part_copy(target):
        return remote(
            part_out.at[target], part_in.at[row], part_send.at[target], part_recv.at[row], target, col
        )

    def halves_of(values):
        left, right = values[:, :share], values[:, share:]
        return jnp.where(member == 0, left, right), jnp.where(member == 0, right, left)

    far, near = flipped(order[0]), order[1:]
    far_copy = part_copy(far * members + member)
    pair_copy = remote(pair_out, pair_in, pair_send, pair_recv, partner, col)

    far_own, far_other = halves_of(product(far))
    pair_out[...] = far_other
    pair_copy.start()
    for mask in near:
        group = flipped(mask)
        values = product(group)
        for c in range(members):
            part_out[group * members + c] = values[:, c * share:(c + 1) * share].astype(BF16)
            part_copy(group * members + c).start()

    total, other = halves_of(product(mine))
    part_out[partner] = other.astype(BF16)
    part_copy(partner).start()
    pair_copy.wait_recv()
    part_out[far * members + member] = (far_own + pair_in[...]).astype(BF16)
    far_copy.start()

    def take(source):
        remote(part_out.at[0], part_in.at[source], part_send.at[0], part_recv.at[source], row, col).wait_recv()
        return part_in[source].astype(F32)

    total += take(partner)
    for mask in near:
        for c in range(members):
            total += take(flipped(mask) * members + c)
    total += take(far * members + member)

    out[...] = total

    for c in range(lead):
        @pl.when(member == c)
        def _():
            @pl.when(below)
            def _():
                move_fac(c).wait_send()
                move_inv(c).wait_send()

    for c in range(members):
        @pl.when(jnp.logical_and(first, member == c))
        def _():
            for i in range(len(p_targets)):
                send_p(c, i).wait_send()

    @pl.when(sends_fit)
    def _():
        send_fit.wait_send()

    @pl.when(role(1, 0))
    def _():
        send_t(0, 3, 0).wait_send()
        send_s(2, 1).wait_send()
        send_t(1, 3, 1).wait_send()
        for z in range(n_pair):
            for c in range(members):
                last_copy(c, z).wait_send()
        spread_rounded(1, False)

    @pl.when(role(2, 0))
    def _():
        send_u(2).wait_send()
        send_y().wait_send()

    @pl.when(jnp.logical_or(role(3, 0), role(3, 1)))
    def _():
        send_u(3).wait_send()
        send_y().wait_send()

    @pl.when(role(2, 1))
    def _():
        send_s(3, 2).wait_send()
        send_v(1, 0).wait_send()
        spread_rounded(2, False)

    @pl.when(role(3, 2))
    def _():
        send_v(2, 1).wait_send()
        send_x().wait_send()
        send_w(0, 3, 1).wait_send()
        send_w(1, 3, 0).wait_send()
        spread_rounded(3, False)

    pair_copy.wait_send()
    far_copy.wait_send()
    part_copy(partner).wait_send()
    for mask in near:
        for c in range(members):
            part_copy(flipped(mask) * members + c).wait_send()


def shards(integrals, densities, screen, factor, diag_inv):
    n_aux, n_pair = lax.axis_size("aux"), lax.axis_size("pair")
    height, width = integrals.shape
    breadth, block = factor.shape[1], diag_inv.shape[1]
    count = densities.shape[0]
    members, pieces = block // height, breadth // height
    share = width // n_aux
    vmem, dma = pltpu.VMEM, pltpu.SemaphoreType.DMA

    def rows(*lead):
        return vmem(lead + (count, height), F32)

    def whole(*lead, kind=F32):
        return vmem(lead + (count, block), kind)

    weights = 2 * block * block * 4 + 10 * block * block * 2
    fits = weights + integrals.size * 2 <= VMEM_ROOM
    if breadth == block and members == 2 and n_pair == SOLVE_BLOCKS and n_aux == 8 and fits:
        body = lead_kernel
        screen_space = pltpu.HBM
        scratch = [
            pltpu.SMEM(screen.shape, screen.dtype), vmem((height, width), BF16), vmem((count, width), BF16),
            vmem((block, block), F32), vmem((block, block), F32),
            *[vmem((block, block), BF16) for _ in range(10)],
            rows(), rows(n_pair, members), whole(kind=P_KIND), whole(n_pair, members, kind=P_KIND),
            whole(), whole(n_pair), whole(kind=S_KIND), whole(kind=S_KIND), whole(2), whole(),
            whole(kind=S_KIND), whole(), whole(), whole(kind=V_KIND), whole(kind=V_KIND),
            whole(), whole(SOLVE_BLOCKS, n_pair),
            whole(), whole(), whole(), vmem((members, count, height), BF16),
            whole(kind=L_KIND), whole(kind=L_KIND), vmem((count, share), F32), vmem((count, share), F32),
            vmem((n_aux, count, share), BF16), vmem((n_aux, count, share), BF16),
            dma((width // STREAM,)), dma((4,)),
            dma, dma((members,)), dma, dma((members,)),
            dma, dma((n_pair, members)), dma((2,)), dma((n_pair, members)), dma, dma((n_pair,)),
            dma, dma, dma((2,)), dma, dma, dma((2,)), dma, dma, dma, dma, dma((SOLVE_BLOCKS, n_pair)),
            dma((members, n_pair)), dma, dma((members, n_pair)), dma, dma, dma,
            dma((n_aux,)), dma((n_aux,)),
        ]
    else:
        body = spread_kernel
        screen_space = pltpu.SMEM
        scratch = [
            vmem((height, width), BF16), vmem((count, width), BF16),
            vmem((height, breadth), F32), vmem((height, block), F32),
            vmem((height, breadth), BF16), vmem((height, breadth), BF16),
            vmem((height, block), BF16), vmem((height, block), BF16),
            rows(), rows(n_pair), rows(), rows(n_pair),
            rows(members), rows(members, pieces), rows(pieces), rows(members, members),
            rows(members), rows(), rows(pieces), rows(n_aux, members),
            vmem((n_aux, count, share), BF16), vmem((n_aux, count, share), BF16),
            dma((width // STREAM,)), dma((3,)),
            dma, dma((n_pair,)), dma, dma((n_pair,)),
            dma((members, n_aux)), dma((members, pieces)),
            dma((members, members)), dma((members, members)),
            dma((n_pair,)), dma, dma((pieces, members)), dma((n_aux, members)),
            dma((n_aux,)), dma((n_aux,)),
        ]
    operands = integrals, densities, screen, factor, diag_inv
    if body is lead_kernel:
        operands = tuple(pltpu.with_memory_space_constraint(x, pltpu.HBM) for x in operands)
    return pl.pallas_call(
        functools.partial(body, n_aux, n_pair),
        out_shape=jax.ShapeDtypeStruct((count, share), F32),
        in_specs=[
            pl.BlockSpec(memory_space=pltpu.HBM),
            pl.BlockSpec(memory_space=pltpu.HBM),
            pl.BlockSpec(memory_space=screen_space),
            pl.BlockSpec(memory_space=pltpu.HBM),
            pl.BlockSpec(memory_space=pltpu.HBM),
        ],
        out_specs=pl.BlockSpec(memory_space=pltpu.VMEM),
        scratch_shapes=scratch,
        compiler_params=pltpu.CompilerParams(
            collective_id=0, has_side_effects=True, vmem_limit_bytes=VMEM_LIMIT if body is lead_kernel else 60 * 2**20
        ),
    )(*operands)


def solution(mesh):
    in_specs = (
        P("aux", "pair"),
        P(None, "pair"),
        P("aux", "pair"),
        P("aux", "pair"),
        P("aux", None),
    )
    out_specs = P(None, ("pair", "aux"))
    return jax.shard_map(shards, mesh=mesh, in_specs=in_specs, out_specs=out_specs, check_vma=False)
```

```python
import functools

import jax
import jax.numpy as jnp
from jax import lax
from jax.experimental import pallas as pl
from jax.experimental.pallas import tpu as pltpu
from jax.sharding import PartitionSpec as P

TILE = 128
SOLVE_BLOCKS = 4
STREAM = 1024
LEAD_STREAM = 2048
VMEM_ROOM = 48 * 2**20
MESH = pl.DeviceIdType.MESH
NN = (((1,), (0,)), ((), ()))
NT = (((1,), (1,)), ((), ()))
F32 = jnp.float32
BF16 = jnp.bfloat16
P_KIND, S_KIND, V_KIND, L_KIND = BF16, BF16, BF16, BF16
VMEM_LIMIT = 44 * 2**20


def split(values):
    high = values.astype(BF16)
    return high, (values - high.astype(F32)).astype(BF16)


def dot_split(values, high, low, dims):
    top, rest = split(values)
    rows = values.shape[0]
    both = lax.dot_general(
        jnp.concatenate([top, rest], 0), high, dims, preferred_element_type=F32
    )
    minor = lax.dot_general(top, low, dims, preferred_element_type=F32)
    return both[:rows] + (both[rows:] + minor)


def spread_kernel(
    n_aux, n_pair,
    integrals, densities, screen, factor, diag_inv, out,
    masked, dens, fac, inv, fac_hi, fac_lo, inv_hi, inv_lo,
    fit_out, fit_in, u_out, u_in, s_out, s_in, s_sum, own_in, resid, coef, v_out, v_in,
    part_out, part_in,
    load_sem, small_sem,
    fit_send, fit_recv, u_send, u_recv, s_send, s_recv, own_send, own_recv,
    coef_send, coef_recv, v_send, v_recv, part_send, part_recv,
):
    height, width = masked.shape
    breadth = fac.shape[1]
    block = inv.shape[1]
    members = block // height
    group = block // breadth
    pieces = breadth // height
    share = width // n_aux
    chunks = width // STREAM

    row = lax.axis_index("aux")
    col = lax.axis_index("pair")
    mine = row // members
    member = lax.rem(row, members)
    column_block = col // group
    column_part = lax.rem(col, group)

    def home_of(k):
        return jnp.maximum(k - 1, 0) * group

    home = home_of(mine)
    is_home = col == home
    below = column_block < mine

    def remote(src, dst, send, recv, aux, pair):
        return pltpu.make_async_remote_copy(
            src_ref=src, dst_ref=dst, send_sem=send, recv_sem=recv,
            device_id={"aux": aux, "pair": pair}, device_id_type=MESH,
        )

    def load(c):
        at = pl.ds(pl.multiple_of(c * STREAM, STREAM), STREAM)
        return pltpu.make_async_copy(integrals.at[:, at], masked.at[:, at], load_sem.at[c])

    load_dens = pltpu.make_async_copy(densities, dens, small_sem.at[0])
    load_fac = pltpu.make_async_copy(factor, fac, small_sem.at[1])
    load_inv = pltpu.make_async_copy(diag_inv, inv, small_sem.at[2])
    load_dens.start()
    for c in range(chunks):
        load(c).start()
    load_inv.start()

    @pl.when(below)
    def _():
        load_fac.start()

    barrier = pltpu.get_barrier_semaphore()
    everyone = n_aux * n_pair
    me = row * n_pair + col

    def greet(i, carry):
        other = lax.rem(me + i, everyone)
        pl.semaphore_signal(
            barrier, inc=1,
            device_id={"aux": other // n_pair, "pair": lax.rem(other, n_pair)},
            device_id_type=MESH,
        )
        return carry

    lax.fori_loop(1, everyone, greet, 0)
    load_dens.wait()

    def fit_step(c, total):
        load(c).wait()
        base = pl.multiple_of(c * STREAM, STREAM)
        for r in range(height // TILE):
            for t in range(STREAM // TILE):
                flag = screen[r, c * (STREAM // TILE) + t].astype(F32)
                at = (pl.ds(r * TILE, TILE), pl.ds(pl.multiple_of(base + t * TILE, TILE), TILE))
                masked[at] = masked[at] * jnp.full((TILE, TILE), flag, F32).astype(BF16)
        span = pl.ds(base, STREAM)
        return total + lax.dot_general(
            dens[:, span], masked[:, span], NT, preferred_element_type=F32
        )

    fitted = lax.fori_loop(0, chunks, fit_step, jnp.zeros((dens.shape[0], height), F32))
    fit_out[...] = fitted
    pl.semaphore_wait(barrier, everyone - 1)

    send_fit = remote(fit_out, fit_in.at[col], fit_send, fit_recv.at[col], row, home)

    @pl.when(jnp.logical_not(is_home))
    def _():
        send_fit.start()

    load_inv.wait()
    high, low = split(inv[...])
    inv_hi[...] = high
    inv_lo[...] = low

    @pl.when(below)
    def _():
        load_fac.wait()
        high, low = split(fac[...])
        fac_hi[...] = high
        fac_lo[...] = low

    @pl.when(below)
    def _():
        for x in range(pieces):
            whole_x = column_part * pieces + x
            for c in range(members):
                @pl.when(whole_x >= c)
                def _():
                    remote(s_out.at[0], s_in.at[c, x], s_send.at[0, 0], s_recv.at[c, x], row, col).wait_recv()
                    if c == 0:
                        s_sum[x] = s_in[c, x]
                    else:
                        s_sum[x] += s_in[c, x]
        known = jnp.concatenate([s_sum[x] for x in range(pieces)], 1)
        u_out[...] = dot_split(known, fac_hi[...], fac_lo[...], NT)

        @pl.when(jnp.logical_not(is_home))
        def _():
            remote(u_out, u_in.at[col], u_send, u_recv.at[col], row, home).start()

    def send_solved(x, start):
        part, piece = x // pieces, x % pieces

        def later(d, carry):
            copy = remote(
                s_out.at[x], s_in.at[member, piece], s_send.at[x, d],
                s_recv.at[member, piece], d, mine * group + part,
            )
            copy.start() if start else copy.wait_send()
            return carry

        lax.fori_loop((mine + 1) * members, n_aux, later, 0)
        for i in range(1, members):
            other = lax.rem(member + i, members)

            @pl.when(other <= x)
            def _():
                copy = remote(
                    s_out.at[x], own_in.at[member, x], own_send.at[x, i],
                    own_recv.at[member, x], mine * members + other, home,
                )
                copy.start() if start else copy.wait_send()

    @pl.when(is_home)
    def _():
        fit_total = fit_out
        for p in range(n_pair):
            @pl.when(p != home)
            def _():
                remote(fit_out, fit_in.at[p], fit_send, fit_recv.at[p], row, col).wait_recv()
                fit_total[...] += fit_in[p]
        for p in range(n_pair):
            @pl.when(jnp.logical_and(p // group < mine, p != home))
            def _():
                remote(u_out, u_in.at[p], u_send, u_recv.at[p], row, col).wait_recv()
                fit_total[...] -= u_in[p]

        @pl.when(below)
        def _():
            fit_total[...] -= u_out[...]

        for x in range(members):
            @pl.when(x >= member)
            def _():
                at = pl.ds(x * height, height)
                s_out[x] = dot_split(fit_total[...], inv_hi[:, at], inv_lo[:, at], NN)
                send_solved(x, True)

        for x in range(members):
            @pl.when(x >= member)
            def _():
                resid[x] = s_out[x]
                for i in range(1, members):
                    other = lax.rem(member + i, members)

                    @pl.when(other <= x)
                    def _():
                        remote(s_out.at[0], own_in.at[other, x], own_send.at[0, 0], own_recv.at[other, x], row, col).wait_recv()
                        resid[x] += own_in[other, x]

        def subtract(i, carry):
            source = n_aux - 1 - i
            for x in range(members):
                @pl.when(x >= member)
                def _():
                    remote(v_out.at[0], v_in.at[source, x], v_send.at[0, 0], v_recv.at[source, x], row, col).wait_recv()
                    resid[x] -= v_in[source, x]
            return carry

        lax.fori_loop(0, n_aux - (mine + 1) * members, subtract, 0)
        for x in reversed(range(members)):
            @pl.when(x >= member)
            def _():
                at = pl.ds(x * height, height)
                term = dot_split(resid[x], inv_hi[:, at], inv_lo[:, at], NT)
                if x == members - 1:
                    coef[...] = term
                else:
                    coef[...] += term

        for i in range(1, n_pair):
            remote(coef, coef, coef_send.at[i], coef_recv, row, lax.rem(col + i, n_pair)).start()

    @pl.when(jnp.logical_not(is_home))
    def _():
        remote(coef, coef, coef_send.at[0], coef_recv, row, col).wait_recv()

    def send_v(x, start):
        whole_x = column_part * pieces + x
        for c in range(members):
            @pl.when(c <= whole_x)
            def _():
                copy = remote(
                    v_out.at[x], v_in.at[row, whole_x], v_send.at[x, c],
                    v_recv.at[row, whole_x], column_block * members + c, home_of(column_block),
                )
                copy.start() if start else copy.wait_send()

    @pl.when(below)
    def _():
        for x in range(pieces):
            at = pl.ds(x * height, height)
            v_out[x] = dot_split(coef[...], fac_hi[:, at], fac_lo[:, at], NN)
            send_v(x, True)

    rounded = coef[...].astype(BF16)

    def product(target):
        span = pl.ds(pl.multiple_of(target * share, TILE), share)
        return lax.dot_general(rounded, masked[:, span], NN, preferred_element_type=F32)

    def part_copy(i):
        target = lax.rem(row + i, n_aux)
        return target, remote(
            part_out.at[target], part_in.at[row], part_send.at[target], part_recv.at[row], target, col
        )

    def give(i, carry):
        target, copy = part_copy(i)
        part_out[target] = product(target).astype(BF16)
        copy.start()
        return carry

    lax.fori_loop(1, n_aux, give, 0)
    total = product(row)

    def take(i, total):
        source = lax.rem(row + n_aux - i, n_aux)
        remote(part_out.at[0], part_in.at[source], part_send.at[0], part_recv.at[source], row, col).wait_recv()
        return total + part_in[source].astype(F32)

    out[...] = lax.fori_loop(1, n_aux, take, total)

    @pl.when(jnp.logical_not(is_home))
    def _():
        send_fit.wait_send()

        @pl.when(below)
        def _():
            remote(u_out, u_in.at[col], u_send, u_recv.at[col], row, home).wait_send()

    @pl.when(is_home)
    def _():
        for x in range(members):
            @pl.when(x >= member)
            def _():
                send_solved(x, False)
        for i in range(1, n_pair):
            remote(coef, coef, coef_send.at[i], coef_recv, row, lax.rem(col + i, n_pair)).wait_send()

    @pl.when(below)
    def _():
        for x in range(pieces):
            send_v(x, False)

    def sent(i, carry):
        part_copy(i)[1].wait_send()
        return carry

    lax.fori_loop(1, n_aux, sent, 0)


def dot_two(values, high, low, dims):
    return lax.dot_general(values, high, dims, preferred_element_type=F32) + lax.dot_general(
        values, low, dims, preferred_element_type=F32
    )


def apply(values, high, low, dims):
    return (dot_two if values.dtype == BF16 else dot_split)(values, high, low, dims)


def lead_kernel(
    n_aux, n_pair,
    integrals, densities, screen, factor, diag_inv, out,
    flags, masked, dens, fac, inv, fac_hi, fac_lo, inv_hi, inv_lo, inv_t_hi, inv_t_lo,
    step_hi, step_lo, step_t_hi, step_t_lo,
    fit_out, fit_in, p_out, p_in, u_out, u_in, s_out, s_in, t_out, t_in, x_out, w_out, w_in, v_out, v_in, y_out, y_in,
    resid, solved, start, rounded, last_out, last_in, pair_out, pair_in, part_out, part_in,
    load_sem, small_sem, fac_send, fac_recv, inv_send, inv_recv,
    fit_send, fit_recv, p_send, p_recv, u_send, u_recv, s_send, s_recv, t_send, t_recv, x_send, w_send, w_recv,
    v_send, v_recv, y_send, y_recv, round_send, round_recv, last_send, last_recv, pair_send, pair_recv, part_send, part_recv,
):
    height, width = masked.shape
    block = inv.shape[1]
    count = dens.shape[0]
    members = block // height
    share = width // n_aux
    chunks = width // STREAM
    wide = LEAD_STREAM // STREAM
    tail = chunks - wide
    strips = height // TILE

    row = lax.axis_index("aux")
    col = lax.axis_index("pair")
    mine = row // members
    member = lax.rem(row, members)
    lead = members - 1
    lead_row = mine * members + lead
    is_lead = member == lead
    first = mine == 0
    later = mine > 0
    home = jnp.maximum(mine - 1, 0)
    at_home = jnp.logical_and(later, col == home)
    below = col < mine

    def chip(k, z):
        return jnp.logical_and(mine == k, col == z)

    def role(k, z):
        return jnp.logical_and(is_lead, chip(k, z))

    lead_home = jnp.logical_and(is_lead, at_home)
    lead_below = jnp.logical_and(is_lead, below)

    def remote(src, dst, send, recv, aux, pair):
        return pltpu.make_async_remote_copy(
            src_ref=src, dst_ref=dst, send_sem=send, recv_sem=recv,
            device_id={"aux": aux, "pair": pair}, device_id_type=MESH,
        )

    def to_lead(src, dst, send, recv, k, z):
        return remote(src, dst, send, recv, k * members + lead, z)

    def load(c):
        at = pl.ds(pl.multiple_of(c * STREAM, STREAM), STREAM)
        return pltpu.make_async_copy(integrals.at[:, at], masked.at[:, at], load_sem.at[c])

    own = pl.ds(lead * height, height)
    load_dens = pltpu.make_async_copy(densities, dens, small_sem.at[0])
    load_fac = pltpu.make_async_copy(factor, fac.at[own], small_sem.at[1])
    load_inv = pltpu.make_async_copy(diag_inv, inv.at[own], small_sem.at[2])
    load_flags = pltpu.make_async_copy(screen, flags, small_sem.at[3])

    def move_fac(c):
        return remote(factor, fac.at[pl.ds(c * height, height)], fac_send, fac_recv.at[c], lead_row, col)

    def move_inv(c):
        right = pl.ds(c * height, block - c * height)
        return remote(
            diag_inv.at[:, right], inv.at[pl.ds(c * height, height), right],
            inv_send, inv_recv.at[c], lead_row, col,
        )

    def load_start(c):
        right = pl.ds(c * height, block - c * height)
        return pltpu.make_async_copy(diag_inv.at[:, right], inv.at[own, right], small_sem.at[2])

    load_flags.start()
    load_dens.start()
    for c in range(chunks):
        load(c).start()
    for c in range(members):
        @pl.when(jnp.logical_and(first, member == c))
        def _():
            load_start(c).start()


    @pl.when(lead_below)
    def _():
        load_fac.start()
        load_inv.start()

    barrier = pltpu.get_barrier_semaphore()

    def greet(k, c, z):
        pl.semaphore_signal(
            barrier, inc=1, device_id={"aux": k * members + c, "pair": z}, device_id_type=MESH
        )

    c_one, c_two, c_three = role(1, 0), role(2, 1), role(3, 2)
    lead_aside = jnp.logical_and(lead_below, jnp.logical_not(at_home))

    @pl.when(jnp.logical_or(c_one, role(2, 0)))
    def _():
        for c in range(members):
            for z in range(n_pair):
                greet(0, c, z)

    @pl.when(lead_home)
    def _():
        for c in range(members):
            for i in range(n_pair):
                if c != lead or i:
                    greet(mine, c, lax.rem(col + i, n_pair))

    @pl.when(lead_aside)
    def _():
        for c in range(lead):
            greet(mine, c, col)

    @pl.when(jnp.logical_or(c_two, jnp.logical_and(lead_aside, mine == 3)))
    def _():
        greet(1, lead, 0)

    @pl.when(c_three)
    def _():
        greet(2, lead, 1)

    gives = jnp.logical_and(jnp.logical_not(is_lead), below)
    greeted = (
        jnp.where(first, 2, 0)
        + jnp.where(jnp.logical_and(later, jnp.logical_not(lead_home)), 1, 0)
        + jnp.where(jnp.logical_and(gives, jnp.logical_not(at_home)), 1, 0)
        + jnp.where(c_one, 3, 0)
        + jnp.where(c_two, 1, 0)
    )

    @pl.when(gives)
    def _():
        pl.semaphore_wait(barrier, greeted)

    for c in range(lead):
        @pl.when(jnp.logical_and(gives, member == c))
        def _():
            move_fac(c).start()
            move_inv(c).start()

    load_flags.wait()
    load_dens.wait()

    def flag_of(r, t):
        return flags[r, t].astype(F32)

    def fit_step(c, steps, sums):
        size = steps * STREAM
        base = pl.multiple_of(c * STREAM, STREAM)
        kept = []
        for r in range(strips):
            tiles = []
            for t in range(size // TILE):
                at = pl.ds(pl.multiple_of(base + t * TILE, TILE), TILE)
                flag = flag_of(r, c * (STREAM // TILE) + t)
                tiles.append(dens[:, at] * jnp.full((count, TILE), flag, F32).astype(BF16))
            kept.append(jnp.concatenate(tiles, 1))
        for i in range(steps):
            load(c + i).wait()
        return tuple(
            sums[r] + lax.dot_general(
                kept[r], masked[pl.ds(r * TILE, TILE), pl.ds(base, size)], NT,
                preferred_element_type=F32,
            )
            for r in range(strips)
        )

    sums = lax.fori_loop(
        0, tail // wide, lambda i, sums: fit_step(i * wide, wide, sums),
        tuple(jnp.zeros((count, TILE), F32) for _ in range(strips)),
    )
    for c in range(members):
        @pl.when(jnp.logical_and(first, member == c))
        def _():
            right = pl.ds(c * height, block - c * height)
            load_start(c).wait()
            inv_hi[own, right], inv_lo[own, right] = split(inv[own, right])

    sums = fit_step(tail, wide, sums)
    for r in range(strips):
        fit_out[:, pl.ds(r * TILE, TILE)] = sums[r]

    p_targets = ((1, 0), (2, 0))

    def send_p(c, i):
        right = pl.ds(c * height, block - c * height)
        return to_lead(
            p_out.at[:, right], p_in.at[col, c, :, right], p_send.at[i], p_recv.at[col, c], *p_targets[i]
        )

    for c in range(members):
        @pl.when(jnp.logical_and(first, member == c))
        def _():
            right = pl.ds(c * height, block - c * height)
            p_out[:, right] = dot_split(
                fit_out[...], inv_hi[own, right], inv_lo[own, right], NN
            ).astype(p_out.dtype)

    @pl.when(jnp.logical_not(jnp.logical_or(gives, c_three)))
    def _():
        pl.semaphore_wait(barrier, greeted)


    for c in range(members):
        @pl.when(jnp.logical_and(first, member == c))
        def _():
            for i in range(len(p_targets)):
                send_p(c, i).start()

    send_fit = remote(
        fit_out, fit_in.at[col, member], fit_send, fit_recv.at[col, member], lead_row, home
    )
    sends_fit = jnp.logical_and(later, jnp.logical_not(lead_home))

    @pl.when(sends_fit)
    def _():
        send_fit.start()

    def mask_step(c, carry):
        base = pl.multiple_of(c * STREAM, STREAM)
        for r in range(strips):
            for t in range(STREAM // TILE):
                flag = flag_of(r, c * (STREAM // TILE) + t)
                at = (pl.ds(r * TILE, TILE), pl.ds(pl.multiple_of(base + t * TILE, TILE), TILE))
                masked[at] = masked[at] * jnp.full((TILE, TILE), flag, F32).astype(BF16)
        return carry

    lax.fori_loop(0, chunks, mask_step, 0)

    for c in range(members):
        @pl.when(jnp.logical_and(first, member == c))
        def _():
            right = pl.ds(c * height, block - c * height)
            inv_t_hi[right, :height], inv_t_lo[right, :height] = split(inv[own, right].T)

    @pl.when(lead_below)
    def _():
        load_fac.wait()
        for c in range(lead):
            move_fac(c).wait_recv()
        fac_hi[...], fac_lo[...] = split(fac[...])
        load_inv.wait()
        for c in range(lead):
            move_inv(c).wait_recv()
        inv_hi[...], inv_lo[...] = split(inv[...])

    def prepare_back():
        inv_t_hi[...], inv_t_lo[...] = split(inv[...].T)
        whole = lax.dot_general(inv_t_hi[...], fac_hi[...], NN, preferred_element_type=F32)
        whole += lax.dot_general(inv_t_lo[...], fac_hi[...], NN, preferred_element_type=F32)
        whole += lax.dot_general(inv_t_hi[...], fac_lo[...], NN, preferred_element_type=F32)
        step_t_hi[...], step_t_lo[...] = split(whole)
        return whole

    def prepare_ahead():
        whole = prepare_back()
        step_hi[...], step_lo[...] = split(whole.T)

    def turn_fac():
        step_hi[...], step_lo[...] = split(fac[...].T)

    def gather_fit():
        resid[:, own] = fit_out[...]
        for c in range(lead):
            for p in range(n_pair):
                @pl.when(p == home)
                def _():
                    remote(fit_out, fit_in.at[p, c], fit_send, fit_recv.at[p, c], row, col).wait_recv()
                    resid[:, pl.ds(c * height, height)] = fit_in[p, c]
        for p in range(n_pair):
            for c in range(members):
                @pl.when(p != home)
                def _():
                    remote(fit_out, fit_in.at[p, c], fit_send, fit_recv.at[p, c], row, col).wait_recv()
                    resid[:, pl.ds(c * height, height)] += fit_in[p, c]

    def gather_start():
        for p in range(n_pair):
            for c in range(members):
                right = pl.ds(c * height, block - c * height)
                remote(
                    p_out.at[:, right], p_in.at[p, c, :, right], p_send.at[0], p_recv.at[p, c], row, col
                ).wait_recv()
        for c in range(members):
            at = pl.ds(c * height, height)
            sum_p = p_in[0, 0, :, at].astype(F32)
            for p in range(n_pair):
                for d in range(c + 1):
                    if p or d:
                        sum_p += p_in[p, d, :, at].astype(F32)
            start[:, at] = sum_p

    def send_s(k, z):
        return to_lead(s_out, s_in, s_send, s_recv, k, z)

    def send_x():
        return to_lead(x_out, s_in, x_send, s_recv, 2, 0)

    def send_t(slot, k, z):
        return to_lead(t_out.at[slot], t_in, t_send.at[slot], t_recv, k, z)

    def send_u(k):
        return to_lead(u_out, u_in.at[col], u_send, u_recv.at[col], k, k - 1)

    def send_v(k, z):
        return to_lead(v_out, v_in, v_send, v_recv, k, z)

    def send_y():
        return to_lead(y_out, y_in.at[mine, col], y_send, y_recv.at[mine, col], 1, 0)

    def send_w(i, k, z):
        return to_lead(w_out, w_in, w_send.at[i], w_recv, k, z)

    def wait_s():
        send_s(0, 0).wait_recv()

    def take_u(p):
        remote(u_out, u_in.at[p], u_send, u_recv.at[p], row, col).wait_recv()
        resid[...] -= u_in[p].astype(F32)

    def take_v():
        remote(v_out, v_in, v_send, v_recv, row, col).wait_recv()
        return v_in[...].astype(F32)

    def take_y(k, z):
        remote(y_out, y_in.at[k, z], y_send, y_recv.at[k, z], row, col).wait_recv()
        return y_in[k, z]

    def wait_w():
        send_w(0, 0, 0).wait_recv()

    def round_copy(k, c, i, z):
        return remote(
            rounded.at[c], rounded.at[c], round_send.at[c, i], round_recv, k * members + c, lax.rem(z + i, n_pair)
        )

    def spread_rounded(k, go):
        for i in reversed(range(n_pair)):
            for c in range(members):
                if c != lead or i:
                    copy = round_copy(k, c, i, k - 1)
                    copy.start() if go else copy.wait_send()

    def finish(k, values):
        coef = dot_split(values, inv_t_hi[...], inv_t_lo[...], NN)
        for c in range(members):
            rounded[c] = coef[:, c * height:(c + 1) * height].astype(BF16)
        spread_rounded(k, True)

    def last_copy(c, z):
        right = pl.ds(c * height, block - c * height)
        return remote(
            last_out.at[:, right], last_in.at[:, right], last_send.at[c, z], last_recv, c, z
        )

    @pl.when(role(1, 0))
    def _():
        turn_fac()
        gather_fit()
        gather_start()
        t_out[0] = start[...]
        send_t(0, 3, 0).start()
        resid[...] -= dot_split(start[...], step_hi[...], step_lo[...], NN)
        solved[...] = dot_split(resid[...], inv_hi[...], inv_lo[...], NN)
        s_out[...] = solved[...].astype(s_out.dtype)
        t_out[1] = solved[...]
        send_s(2, 1).start()
        send_t(1, 3, 1).start()
        prepare_back()
        solved[...] -= take_y(3, 1)
        start[...] -= take_y(3, 0)
        solved[...] -= take_v()
        back = dot_split(solved[...], step_t_hi[...], step_t_lo[...], NN)
        last_out[...] = (start[...] - take_y(2, 0) - back).astype(last_out.dtype)
        for z in reversed(range(n_pair)):
            for c in range(members):
                last_copy(c, z).start()
        finish(1, solved[...])

    @pl.when(role(2, 0))
    def _():
        turn_fac()
        gather_start()
        u_out[...] = dot_split(start[...], step_hi[...], step_lo[...], NN)
        send_u(2).start()
        prepare_back()
        wait_s()
        y_out[...] = apply(s_in[...], step_t_hi[...], step_t_lo[...], NN)
        send_y().start()

    @pl.when(jnp.logical_or(role(3, 0), role(3, 1)))
    def _():
        prepare_ahead()
        send_t(0, 0, 0).wait_recv()
        u_out[...] = dot_split(t_in[...], step_hi[...], step_lo[...], NN)
        send_u(3).start()
        wait_w()
        y_out[...] = dot_split(w_in[...], step_t_hi[...], step_t_lo[...], NN)
        send_y().start()

    @pl.when(role(2, 1))
    def _():
        prepare_ahead()
        gather_fit()
        take_u(0)
        resid[...] = dot_split(resid[...], inv_hi[...], inv_lo[...], NN)
        wait_s()
        solved[...] = resid[...] - apply(s_in[...], step_hi[...], step_lo[...], NN)
        s_out[...] = solved[...].astype(s_out.dtype)
        send_s(3, 2).start()
        solved[...] -= take_v()
        v_out[...] = dot_split(solved[...], step_t_hi[...], step_t_lo[...], NN).astype(v_out.dtype)
        send_v(1, 0).start()
        finish(2, solved[...])

    @pl.when(role(3, 2))
    def _():
        prepare_ahead()
        gather_fit()
        resid[...] = dot_split(resid[...], inv_hi[...], inv_lo[...], NN)
        take_u(0)
        take_u(1)
        wait_s()
        solved[...] = resid[...] - apply(s_in[...], step_hi[...], step_lo[...], NN)
        w_out[...] = solved[...]
        send_w(0, 3, 1).start()
        send_w(1, 3, 0).start()
        back = dot_split(solved[...], step_t_hi[...], step_t_lo[...], NN)
        v_out[...] = back.astype(v_out.dtype)
        send_v(2, 1).start()
        x_out[...] = (s_in[...].astype(F32) - back).astype(x_out.dtype)
        send_x().start()
        coef = dot_split(solved[...], inv_t_hi[...], inv_t_lo[...], NN)
        for c in range(members):
            rounded[c] = coef[:, c * height:(c + 1) * height].astype(BF16)
        spread_rounded(3, True)

    @pl.when(jnp.logical_and(later, jnp.logical_not(lead_home)))
    def _():
        remote(rounded.at[0], rounded.at[0], round_send.at[0, 0], round_recv, row, col).wait_recv()

    for c in range(members):
        @pl.when(jnp.logical_and(first, member == c))
        def _():
            right = pl.ds(c * height, block - c * height)
            remote(
                last_out.at[:, right], last_in.at[:, right], last_send.at[c, 0], last_recv, row, col
            ).wait_recv()
            rounded[c] = apply(
                last_in[:, right], inv_t_hi[right, :height], inv_t_lo[right, :height], NN
            ).astype(BF16)

    mine_rounded = rounded[member]

    span = members * share

    def product(group):
        at = pl.ds(pl.multiple_of(group * span, TILE), span)
        return lax.dot_general(mine_rounded, masked[:, at], NN, preferred_element_type=F32)

    def flipped(mask):
        group, unit = 0, 1
        while unit * members < n_aux:
            digit = lax.rem(mine // unit, 2)
            group = group + unit * (1 - digit if mask & unit else digit)
            unit *= 2
        return group

    order = sorted(range(1, n_aux // members), key=lambda m: -bin(m).count("1"))
    partner = mine * members + 1 - member

    def part_copy(target):
        return remote(
            part_out.at[target], part_in.at[row], part_send.at[target], part_recv.at[row], target, col
        )

    def halves_of(values):
        left, right = values[:, :share], values[:, share:]
        return jnp.where(member == 0, left, right), jnp.where(member == 0, right, left)

    far, near = flipped(order[0]), order[1:]
    far_copy = part_copy(far * members + member)
    pair_copy = remote(pair_out, pair_in, pair_send, pair_recv, partner, col)

    far_own, far_other = halves_of(product(far))
    pair_out[...] = far_other
    pair_copy.start()
    for mask in near:
        group = flipped(mask)
        values = product(group)
        for c in range(members):
            part_out[group * members + c] = values[:, c * share:(c + 1) * share].astype(BF16)
            part_copy(group * members + c).start()

    total, other = halves_of(product(mine))
    part_out[partner] = other.astype(BF16)
    part_copy(partner).start()
    pair_copy.wait_recv()
    part_out[far * members + member] = (far_own + pair_in[...]).astype(BF16)
    far_copy.start()

    def take(source):
        remote(part_out.at[0], part_in.at[source], part_send.at[0], part_recv.at[source], row, col).wait_recv()
        return part_in[source].astype(F32)

    total += take(partner)
    for mask in near:
        for c in range(members):
            total += take(flipped(mask) * members + c)
    total += take(far * members + member)

    out[...] = total

    for c in range(lead):
        @pl.when(member == c)
        def _():
            @pl.when(below)
            def _():
                move_fac(c).wait_send()
                move_inv(c).wait_send()

    for c in range(members):
        @pl.when(jnp.logical_and(first, member == c))
        def _():
            for i in range(len(p_targets)):
                send_p(c, i).wait_send()

    @pl.when(sends_fit)
    def _():
        send_fit.wait_send()

    @pl.when(role(1, 0))
    def _():
        send_t(0, 3, 0).wait_send()
        send_s(2, 1).wait_send()
        send_t(1, 3, 1).wait_send()
        for z in range(n_pair):
            for c in range(members):
                last_copy(c, z).wait_send()
        spread_rounded(1, False)

    @pl.when(role(2, 0))
    def _():
        send_u(2).wait_send()
        send_y().wait_send()

    @pl.when(jnp.logical_or(role(3, 0), role(3, 1)))
    def _():
        send_u(3).wait_send()
        send_y().wait_send()

    @pl.when(role(2, 1))
    def _():
        send_s(3, 2).wait_send()
        send_v(1, 0).wait_send()
        spread_rounded(2, False)

    @pl.when(role(3, 2))
    def _():
        send_v(2, 1).wait_send()
        send_x().wait_send()
        send_w(0, 3, 1).wait_send()
        send_w(1, 3, 0).wait_send()
        spread_rounded(3, False)

    pair_copy.wait_send()
    far_copy.wait_send()
    part_copy(partner).wait_send()
    for mask in near:
        for c in range(members):
            part_copy(flipped(mask) * members + c).wait_send()


def shards(integrals, densities, screen, factor, diag_inv):
    n_aux, n_pair = lax.axis_size("aux"), lax.axis_size("pair")
    height, width = integrals.shape
    breadth, block = factor.shape[1], diag_inv.shape[1]
    count = densities.shape[0]
    members, pieces = block // height, breadth // height
    share = width // n_aux
    vmem, dma = pltpu.VMEM, pltpu.SemaphoreType.DMA

    def rows(*lead):
        return vmem(lead + (count, height), F32)

    def whole(*lead, kind=F32):
        return vmem(lead + (count, block), kind)

    weights = 2 * block * block * 4 + 10 * block * block * 2
    fits = weights + integrals.size * 2 <= VMEM_ROOM
    if breadth == block and members == 2 and n_pair == SOLVE_BLOCKS and n_aux == 8 and fits:
        body = lead_kernel
        screen_space = pltpu.HBM
        scratch = [
            pltpu.SMEM(screen.shape, screen.dtype), vmem((height, width), BF16), vmem((count, width), BF16),
            vmem((block, block), F32), vmem((block, block), F32),
            *[vmem((block, block), BF16) for _ in range(10)],
            rows(), rows(n_pair, members), whole(kind=P_KIND), whole(n_pair, members, kind=P_KIND),
            whole(), whole(n_pair), whole(kind=S_KIND), whole(kind=S_KIND), whole(2), whole(),
            whole(kind=S_KIND), whole(), whole(), whole(kind=V_KIND), whole(kind=V_KIND),
            whole(), whole(SOLVE_BLOCKS, n_pair),
            whole(), whole(), whole(), vmem((members, count, height), BF16),
            whole(kind=L_KIND), whole(kind=L_KIND), vmem((count, share), F32), vmem((count, share), F32),
            vmem((n_aux, count, share), BF16), vmem((n_aux, count, share), BF16),
            dma((width // STREAM,)), dma((4,)),
            dma, dma((members,)), dma, dma((members,)),
            dma, dma((n_pair, members)), dma((2,)), dma((n_pair, members)), dma, dma((n_pair,)),
            dma, dma, dma((2,)), dma, dma, dma((2,)), dma, dma, dma, dma, dma((SOLVE_BLOCKS, n_pair)),
            dma((members, n_pair)), dma, dma((members, n_pair)), dma, dma, dma,
            dma((n_aux,)), dma((n_aux,)),
        ]
    else:
        body = spread_kernel
        screen_space = pltpu.SMEM
        scratch = [
            vmem((height, width), BF16), vmem((count, width), BF16),
            vmem((height, breadth), F32), vmem((height, block), F32),
            vmem((height, breadth), BF16), vmem((height, breadth), BF16),
            vmem((height, block), BF16), vmem((height, block), BF16),
            rows(), rows(n_pair), rows(), rows(n_pair),
            rows(members), rows(members, pieces), rows(pieces), rows(members, members),
            rows(members), rows(), rows(pieces), rows(n_aux, members),
            vmem((n_aux, count, share), BF16), vmem((n_aux, count, share), BF16),
            dma((width // STREAM,)), dma((3,)),
            dma, dma((n_pair,)), dma, dma((n_pair,)),
            dma((members, n_aux)), dma((members, pieces)),
            dma((members, members)), dma((members, members)),
            dma((n_pair,)), dma, dma((pieces, members)), dma((n_aux, members)),
            dma((n_aux,)), dma((n_aux,)),
        ]
    operands = integrals, densities, screen, factor, diag_inv
    if body is lead_kernel:
        operands = tuple(pltpu.with_memory_space_constraint(x, pltpu.HBM) for x in operands)
    return pl.pallas_call(
        functools.partial(body, n_aux, n_pair),
        out_shape=jax.ShapeDtypeStruct((count, share), F32),
        in_specs=[
            pl.BlockSpec(memory_space=pltpu.HBM),
            pl.BlockSpec(memory_space=pltpu.HBM),
            pl.BlockSpec(memory_space=screen_space),
            pl.BlockSpec(memory_space=pltpu.HBM),
            pl.BlockSpec(memory_space=pltpu.HBM),
        ],
        out_specs=pl.BlockSpec(memory_space=pltpu.VMEM),
        scratch_shapes=scratch,
        compiler_params=pltpu.CompilerParams(
            collective_id=0, has_side_effects=True, vmem_limit_bytes=VMEM_LIMIT if body is lead_kernel else 60 * 2**20
        ),
    )(*operands)


def solution(mesh):
    in_specs = (
        P("aux", "pair"),
        P(None, "pair"),
        P("aux", "pair"),
        P("aux", "pair"),
        P("aux", None),
    )
    out_specs = P(None, ("pair", "aux"))
    return jax.shard_map(shards, mesh=mesh, in_specs=in_specs, out_specs=out_specs, check_vma=False)
```
